32 devices in a mesh: rep: 2 (over x), shard: 16 (over z, y, core).
Axes of the slice: x: 2, y: 2, z: 4, core: 2. Of those that a mesh axis runs over, the one named last changes fastest.
Arguments:
- features: float32 [16384, 256], P(('rep', 'shard')), may hold values from -6 to 6
- seed_self: float32 [4096, 256], P(('rep', 'shard')), may hold values from -6 to 6
- hub_ids: int32 [4096], P(('rep', 'shard')), may hold values from 0 to 511
- requests: int32 [512, 32], P(('rep', 'shard')), may hold values from 0 to 511
- counts: int32 [512], P(('rep', 'shard')), may hold values from 1 to 32, as said below
- neighbors: int32 [4096, 15], P(('rep', 'shard')), may hold values from 0 to 767
- weight: float32 [256, 256], replicated, may hold values from -1 to 1
- out_bias: float32 [256], replicated, may hold values from -4 to 4
Outputs:
- embedded: float32 [4096, 256], P(('rep', 'shard'))
The draws below stay inside these ranges and needn't reach their ends.
Inputs may be any that keep to these rules, and one draw needn't show every extreme that they name: `hub_ids`: offsets into the block of features of the same device. `requests`: row d of a device's lists holds offsets into the block of features of the device at shard index d with the same rep index; empty slots hold offsets too. counts[r, s, d] slots of the list from shard index s to shard index d are live, the first ones; for every rep index some destination has 32 live slots from every source. `neighbors`: A code below 256 names a row of the device's hub cache; a code 256 + d * 32 + c names slot c of the device's list to shard index d, and counts only where that slot is live.
All inputs are finite; a program needn't handle non-finite values.
Results may differ from the reference program's by a relative error of at most 0.0003.
Values sent between devices are 32-bit elements; how exact they have to be, the bound alone decides.
A program may use at most 64 MiB of HBM per device.

```python
import jax
import jax.numpy as jnp
from jax import lax

F = 256
FANOUT = 15
CAP = 32
ROWS_DEV = 512
SEEDS_DEV = 128
HUB_DEV = 128
HUBS = 256
SLOTS_DEV = 512
CODES = 768
NODES = 16384
SEEDS = 4096
HUB_SLOTS = 4096
REQ_ROWS = 512
N_REP = 2
N_SHARD = 16


def draw_counts(key, part):
    k_base, k_owner = jax.random.split(jax.random.fold_in(key, 11), 2)
    base_fill = jax.random.randint(k_base, (N_REP, N_SHARD, N_SHARD), CAP // 4, CAP + 1)
    full_owner = jax.random.randint(k_owner, (N_REP, 1, 1), 0, N_SHARD)
    owner_index = lax.broadcasted_iota(jnp.int32, (N_REP, N_SHARD, N_SHARD), 2)
    result = jnp.where(owner_index == full_owner, CAP, base_fill)
    return result.reshape(-1).astype(jnp.int32)


def plant(entries, rng, low, top_value):
    longest = entries.shape.index(max(entries.shape))
    spots = []
    for shift in (0, 1):
        where = [jax.random.randint(jax.random.fold_in(rng, axis), (), 0, length) for axis, length in enumerate(entries.shape)]
        where[longest] = (where[longest] + shift) % entries.shape[longest]
        spots.append(tuple(where))
    return entries.at[spots[0]].set(low).at[spots[1]].set(top_value)


def steps_of(stream_key, extent, shards, low, largest):
    gain = 1.0
    for position, parts in shards:
        steps = jax.random.uniform(jax.random.fold_in(jax.random.fold_in(stream_key, 6), position), (parts,), jnp.float32, low / len(shards), largest / len(shards))
        gain = gain * jnp.repeat(jnp.exp(steps), extent[position] // parts).reshape((-1,) + (1,) * (len(extent) - 1 - position))
    return gain


def bell_draw(rng, extent, deviation, bound, cuts=(), kind=jnp.bfloat16):
    level = steps_of(rng, extent, cuts, -0.22, 0.18) if cuts else 1.0
    values = jax.random.normal(rng, extent, jnp.float32) * deviation * level
    return jnp.minimum(jnp.maximum(values, -bound), bound).astype(kind)


def setup_inputs(seed: int = 0) -> dict:
    seeds = jax.random.split(jax.random.key(seed), 9)
    features = bell_draw(seeds[0], (NODES, F), 1.0, 6.0, ((0, 32),), jnp.float32)
    seed_self = bell_draw(seeds[1], (SEEDS, F), 1.0, 6.0, ((0, 32),), jnp.float32)
    hub_ids = plant(jax.random.randint(seeds[2], (HUB_SLOTS,), 0, ROWS_DEV), jax.random.fold_in(seeds[2], 1), 0, ROWS_DEV - 1).astype(jnp.int32)
    requests = plant(jax.random.randint(seeds[3], (REQ_ROWS, CAP), 0, ROWS_DEV), jax.random.fold_in(seeds[3], 1), 0, ROWS_DEV - 1).astype(jnp.int32)
    counts = draw_counts(jax.random.fold_in(seeds[8], 71), 0)
    neighbors = plant(jax.random.randint(seeds[5], (SEEDS, FANOUT), 0, CODES), jax.random.fold_in(seeds[5], 1), 0, CODES - 1).astype(jnp.int32)
    weight = bell_draw(seeds[6], (F, F), (F // 8) ** -0.5, 1.0, (), jnp.float32)
    out_bias = bell_draw(seeds[7], (F,), 1.0, 4.0, (), jnp.float32)
    return dict(features=features, seed_self=seed_self, hub_ids=hub_ids, requests=requests, counts=counts, neighbors=neighbors, weight=weight, out_bias=out_bias)


def reference(features, seed_self, hub_ids, requests, counts, neighbors, weight, out_bias):
    blocks = features.reshape(N_REP, N_SHARD, ROWS_DEV, F)
    hub_index = hub_ids.reshape(N_REP, N_SHARD, HUB_DEV)
    request_index = requests.reshape(N_REP, N_SHARD, N_SHARD, CAP)
    fill_counts = counts.reshape(N_REP, N_SHARD, N_SHARD)
    neighbor_codes = neighbors.reshape(N_REP * N_SHARD, SEEDS_DEV, FANOUT)
    own_rows = seed_self.reshape(N_REP * N_SHARD, SEEDS_DEV, F)
    rep_iota = jnp.arange(N_REP, dtype=jnp.int32)[:, None]
    shard_iota = jnp.arange(N_SHARD, dtype=jnp.int32)[:, None]
    slot_iota = jnp.arange(CAP, dtype=jnp.int32)[None, :]

    def per_device(device_index):
        rep_pos = device_index // N_SHARD
        shard_pos = device_index % N_SHARD
        hub_cache = blocks[rep_iota, shard_pos, hub_index[:, shard_pos]].reshape(HUBS, F)
        fetched = blocks[rep_pos, shard_iota, request_index[rep_pos, shard_pos]].reshape(SLOTS_DEV, F)
        source = jnp.concatenate([hub_cache, fetched], axis=0)
        slot_live = (slot_iota < fill_counts[rep_pos, shard_pos][:, None]).astype(jnp.float32)
        live = jnp.concatenate([jnp.ones((HUBS,), jnp.float32), slot_live.reshape(SLOTS_DEV)])
        codes = neighbor_codes[device_index]
        picked = source[codes]
        weights = live[codes]
        total = own_rows[device_index] + jnp.sum(picked * weights[:, :, None], axis=1)
        taken = 1.0 + jnp.sum(weights, axis=1)
        mean_rows = total / taken[:, None]
        product = jnp.dot(mean_rows, weight, precision=lax.Precision.HIGHEST, preferred_element_type=jnp.float32)
        return jnp.maximum(product + out_bias, 0.0)

    result = lax.map(per_device, jnp.arange(N_REP * N_SHARD, dtype=jnp.int32))
    return result.reshape(SEEDS, F)
```

```python
import functools

import jax
import jax.numpy as jnp
from jax import lax
from jax.experimental import pallas as pl
from jax.experimental.pallas import tpu as pltpu
from jax.sharding import PartitionSpec as P

LANES = 128


def halves(values):
    high = values.astype(jnp.bfloat16)
    low = (values - high.astype(jnp.float32)).astype(jnp.bfloat16)
    return high, low


def dot(left, right):
    return jnp.dot(left, right, preferred_element_type=jnp.float32)


def columns_of(rows):
    count = rows.shape[0]
    if count < LANES:
        rows = jnp.concatenate([rows, jnp.zeros((LANES - count, LANES), rows.dtype)], axis=0)
    return rows.T


def kernel(
    n, reps, feat_hbm, self_hbm, hub_hbm, req_hbm, cnt_hbm, nbr_hbm, weight_hbm, out_ref,
    feat, own, weight, hub_ref, req_ref, cnt_ref, nbr_ref, table, req_recv, gathered, fetched, hubs, slot_tally,
    local_sem, ask_sem, ask_recv_sem, row_send_sem, row_recv_sem, hub_send_sem, hub_recv_sem, known,
):
    me = lax.axis_index("shard")
    rep = lax.axis_index("rep")
    rows, width = feat.shape
    cap = req_ref.shape[1]
    hub_dev = hub_ref.shape[1]
    fanout, seeds = nbr_ref.shape
    hub_total = hub_dev * reps
    quarter = n // 4
    block, place = me // quarter, lax.rem(me, quarter)
    side = block // 2
    inner = lax.rem(block + side, 2)
    is_inner = inner == 1
    near = 1 + lax.rem(block, 2)
    edge = 3 * side
    third = 2 - lax.rem(block, 2)
    far = 3 - edge
    turns = [lax.rem(place + q, quarter) for q in range(quarter)]

    loads = [
        pltpu.make_async_copy(src, dst, local_sem.at[i])
        for i, (src, dst) in enumerate(
            (
                (req_hbm, req_ref),
                (feat_hbm, feat),
                (hub_hbm, hub_ref),
                (nbr_hbm, nbr_ref),
                (cnt_hbm, cnt_ref),
                (self_hbm, own),
                (weight_hbm, weight),
            )
        )
    ]
    for load in loads:
        load.start()

    barrier = pltpu.get_barrier_semaphore()

    def greet(peer_block, places):
        for spot in places:
            pl.semaphore_signal(barrier, inc=1, device_id={"shard": peer_block * quarter + spot})

    greet(near, turns)

    @pl.when(is_inner)
    def _():
        greet(edge, turns)

    greet(block, turns[1:])
    for off in range(1, reps):
        pl.semaphore_signal(barrier, inc=1, device_id={"rep": lax.rem(rep + off, reps)})

    loads[0].wait()
    lists = jnp.concatenate([req_ref[...], jnp.zeros((n, LANES - cap), jnp.int32)], axis=1)
    table[...] = lists.reshape(4, quarter, 1, LANES)
    req_recv[block, place] = table[block, place]

    loads[1].wait()
    high, low = halves(feat[...])
    row_iota = lax.broadcasted_iota(jnp.int32, (LANES, rows), 1)

    loads[2].wait()
    hub_columns = columns_of(jnp.broadcast_to(hub_ref[...], (8, hub_dev)))
    pick = (hub_columns[:, 0:1] == row_iota).astype(jnp.float32).astype(jnp.bfloat16)
    hubs[rep] = dot(pick, high) + dot(pick, low)

    pl.semaphore_wait(barrier, quarter - 1 + quarter + quarter * inner + reps - 1)

    def asks(to_block, places):
        return [
            pltpu.make_async_remote_copy(
                src_ref=table.at[to_block, spot],
                dst_ref=req_recv.at[block, place],
                send_sem=ask_sem.at[to_block, spot],
                recv_sem=ask_recv_sem.at[block, place],
                device_id={"shard": to_block * quarter + spot},
            )
            for spot in places
        ]

    def start(copies):
        for copy in copies:
            copy.start()

    def sent(copies):
        for copy in copies:
            copy.wait_send()

    near_asks = asks(near, turns)
    own_asks = asks(block, turns[1:])
    edge_asks = asks(edge, turns)
    far_asks = asks(far, turns)
    two_asks = asks(third, turns)

    def tell(to_block, slot):
        pl.semaphore_signal(known.at[slot], inc=1, device_id={"shard": to_block * quarter + place})

    start(near_asks)

    @pl.when(is_inner)
    def _():
        tell(edge, 0)
        tell(near, 0)
        start(edge_asks)

    start(own_asks)
    shares = []
    for off in range(1, reps):
        share = pltpu.make_async_remote_copy(
            src_ref=hubs.at[rep],
            dst_ref=hubs.at[rep],
            send_sem=hub_send_sem.at[off],
            recv_sem=hub_recv_sem.at[rep],
            device_id={"rep": lax.rem(rep + off, reps)},
        )
        share.start()
        shares.append(share)
    pl.semaphore_wait(known.at[0], 1)

    @pl.when(is_inner)
    def _():
        tell(edge, 1)
        start(far_asks)

    @pl.when(jnp.logical_not(is_inner))
    def _():
        start(two_asks)
        pl.semaphore_wait(known.at[1], 1)
        start(far_asks)

    batch = min(LANES // cap, quarter)

    def reply_copy(owner_block, spot):
        return pltpu.make_async_remote_copy(
            src_ref=gathered.at[owner_block, spot],
            dst_ref=fetched.at[me],
            send_sem=row_send_sem.at[owner_block, spot],
            recv_sem=row_recv_sem.at[me],
            device_id={"shard": owner_block * quarter + spot},
        )

    def answer(peer_block, places, may_own):
        places = list(places)

        def unless_me(spot, action):
            if may_own:
                pl.when((peer_block != block) | (spot != place))(action)
            else:
                action()

        for spot in places:
            ref = req_recv.at[peer_block, spot]
            unless_me(spot, pltpu.make_async_copy(ref, ref, ask_recv_sem.at[peer_block, spot]).wait)
        request_columns = columns_of(jnp.concatenate([req_recv[peer_block, spot] for spot in places], axis=0))
        for first in range(0, len(places), batch):
            group = places[first : first + batch]
            pick = jnp.concatenate(
                [
                    (request_columns[:cap, i : i + 1] == row_iota[:cap]).astype(jnp.float32)
                    for i in range(first, first + len(group))
                ],
                axis=0,
            ).astype(jnp.bfloat16)
            picked = dot(pick, high) + dot(pick, low)
            for i, q in enumerate(group):
                gathered[peer_block, q] = picked[i * cap : (i + 1) * cap]
        for spot in places:
            unless_me(spot, reply_copy(peer_block, spot).start)

    odd, even, every = range(1, quarter, 2), range(0, quarter, 2), range(quarter)
    @pl.when(is_inner)
    def _():
        answer(near, odd, False)
        answer(far, every, False)
        answer(near, even, False)
        answer(edge, every, False)
        answer(block, every, True)

    @pl.when(jnp.logical_not(is_inner))
    def _():
        answer(near, every, False)
        answer(block, every, True)
        answer(third, every, False)
        answer(far, every, False)

    fetched[me] = gathered[block, place]

    loads[3].wait()
    loads[4].wait()
    code_count = hub_total + n * cap
    code_iota = lax.broadcasted_iota(jnp.int32, (seeds, code_count), 1)
    codes = columns_of(nbr_ref[...])
    tally = jnp.zeros((seeds, code_count), jnp.float32)
    for k in range(fanout):
        tally = tally + (codes[:, k : k + 1] == code_iota).astype(jnp.float32)
    spread = (
        lax.broadcasted_iota(jnp.int32, (n, n * cap), 1) // cap
        == lax.broadcasted_iota(jnp.int32, (n, n * cap), 0)
    ).astype(jnp.float32).astype(jnp.bfloat16)
    fill = jnp.broadcast_to(cnt_ref[...].astype(jnp.float32), (8, n)).astype(jnp.bfloat16)
    slot_fill = dot(fill, spread)[0:1]
    slot_iota = (lax.broadcasted_iota(jnp.int32, (1, n * cap), 1) % cap).astype(jnp.float32)
    slot_live = (slot_iota < slot_fill).astype(jnp.float32)
    hub_tally = tally[:, :hub_total]
    live_tally = tally[:, hub_total:] * slot_live
    taken = 1.0 + jnp.sum(hub_tally, axis=1, keepdims=True) + jnp.sum(live_tally, axis=1, keepdims=True)
    scale = 1.0 / taken
    hub_tally = hub_tally.astype(jnp.bfloat16)
    for b in range(4):
        slot_tally[b] = live_tally[:, b * quarter * cap : (b + 1) * quarter * cap].astype(jnp.bfloat16)

    sent(near_asks + own_asks + far_asks)

    @pl.when(is_inner)
    def _():
        sent(edge_asks)

    @pl.when(jnp.logical_not(is_inner))
    def _():
        sent(two_asks)

    loads[5].wait()
    for off in range(1, reps):
        shares[off - 1].wait_send()
        other = lax.rem(rep + off, reps)
        pltpu.make_async_copy(hubs.at[other], hubs.at[other], hub_recv_sem.at[other]).wait()
    hub_high, hub_low = halves(hubs[...].reshape(hub_total, width))
    total = own[...] + (dot(hub_tally, hub_high) + dot(hub_tally, hub_low))
    loads[6].wait()
    weight_high, weight_low = halves(weight[...])

    for owner_block in (block, block + 1 - 2 * lax.rem(block, 2), 2 - side, far):
        for q, spot in enumerate(turns):
            ref = fetched.at[owner_block * quarter + spot]
            arrival = pltpu.make_async_copy(ref, ref, row_recv_sem.at[owner_block * quarter + spot])
            if q:
                arrival.wait()
            else:
                pl.when(owner_block != block)(arrival.wait)
        row_high, row_low = halves(fetched[pl.ds(owner_block * quarter, quarter)].reshape(quarter * cap, width))
        counted = slot_tally[owner_block]
        total = total + (dot(counted, row_high) + dot(counted, row_low))
    mean_high, mean_low = halves(total * scale)
    out_ref[...] = dot(mean_high, weight_high) + (dot(mean_high, weight_low) + dot(mean_low, weight_high))
    for peer_block in (near, edge, third, far):
        for q, spot in enumerate(turns):
            done = reply_copy(peer_block, spot).wait_send
            if q:
                done()
            else:
                pl.when(peer_block != block)(done)


def local(n, reps, features, seed_self, hub_ids, requests, counts, neighbors, weight, out_bias):
    rows, width = features.shape
    cap = requests.shape[1]
    hub_dev = hub_ids.shape[0]
    seeds, fanout = neighbors.shape
    quarter = n // 4
    hbm = pl.BlockSpec(memory_space=pltpu.HBM)
    dma = pltpu.SemaphoreType.DMA
    product = pl.pallas_call(
        functools.partial(kernel, n, reps),
        out_shape=pltpu.VMEM((seeds, width), jnp.float32),
        in_specs=[hbm] * 7,
        out_specs=pl.BlockSpec(memory_space=pltpu.VMEM),
        scratch_shapes=[
            pltpu.VMEM((rows, width), jnp.float32),
            pltpu.VMEM((seeds, width), jnp.float32),
            pltpu.VMEM(weight.shape, jnp.float32),
            pltpu.VMEM((1, hub_dev), jnp.int32),
            pltpu.VMEM((n, cap), jnp.int32),
            pltpu.VMEM((1, n), jnp.int32),
            pltpu.VMEM((fanout, seeds), jnp.int32),
            pltpu.VMEM((4, quarter, 1, LANES), jnp.int32),
            pltpu.VMEM((4, quarter, 1, LANES), jnp.int32),
            pltpu.VMEM((4, quarter, cap, width), jnp.float32),
            pltpu.VMEM((n, cap, width), jnp.float32),
            pltpu.VMEM((reps, hub_dev, width), jnp.float32),
            pltpu.VMEM((4, seeds, quarter * cap), jnp.bfloat16),
            dma((7,)),
            dma((4, quarter)),
            dma((4, quarter)),
            dma((4, quarter)),
            dma((n,)),
            dma((reps,)),
            dma((reps,)),
            pltpu.SemaphoreType.REGULAR((2,)),
        ],
        compiler_params=pltpu.CompilerParams(collective_id=0, has_side_effects=True),
    )(features, seed_self, hub_ids[None], requests, counts[None], neighbors.T, weight)
    return jnp.maximum(product + out_bias, 0.0)


def solution(mesh):
    return jax.shard_map(
        functools.partial(local, mesh.shape["shard"], mesh.shape["rep"]),
        mesh=mesh,
        in_specs=(
            P(("rep", "shard"), None),
            P(("rep", "shard"), None),
            P(("rep", "shard")),
            P(("rep", "shard"), None),
            P(("rep", "shard")),
            P(("rep", "shard"), None),
            P(),
            P(),
        ),
        out_specs=P(("rep", "shard"), None),
        check_vma=False,
    )
```

```python
import functools

import jax
import jax.numpy as jnp
from jax import lax
from jax.experimental import pallas as pl
from jax.experimental.pallas import tpu as pltpu
from jax.sharding import PartitionSpec as P

LANES = 128
CLIENT, POOL, FEED = 1, 2, 3


def pooled(peer, quarter):
    return peer // quarter == CLIENT and peer % 2 == 0


def halves(values):
    high = values.astype(jnp.bfloat16)
    low = (values - high.astype(jnp.float32)).astype(jnp.bfloat16)
    return high, low


def dot(left, right):
    return jnp.dot(left, right, preferred_element_type=jnp.float32)


def columns_of(rows):
    count = rows.shape[0]
    if count < LANES:
        rows = jnp.concatenate([rows, jnp.zeros((LANES - count, LANES), rows.dtype)], axis=0)
    return rows.T


def kernel(
    n, reps, feat_hbm, self_hbm, hub_hbm, req_hbm, cnt_hbm, nbr_hbm, weight_hbm, out_ref,
    feat, own, weight, hub_ref, req_ref, cnt_ref, nbr_ref, table, req_recv, gathered, fetched, hubs, slot_tally,
    pool, pool_codes, pool_counts, partial, partial_in,
    local_sem, ask_sem, ask_recv_sem, row_send_sem, row_recv_sem, hub_send_sem, hub_recv_sem, present, rep_present,
    pool_sem, code_send_sem, code_recv_sem, partial_sem,
):
    me = lax.axis_index("shard")
    rep = lax.axis_index("rep")
    rows, width = feat.shape
    cap = req_ref.shape[1]
    hub_dev = hub_ref.shape[1]
    fanout, seeds = nbr_ref.shape
    hub_total = hub_dev * reps
    quarter = n // 4
    block, place = me // quarter, lax.rem(me, quarter)

    loads = [
        pltpu.make_async_copy(src, dst, local_sem.at[i])
        for i, (src, dst) in enumerate(
            (
                (req_hbm, req_ref),
                (feat_hbm, feat),
                (hub_hbm, hub_ref),
                (nbr_hbm, nbr_ref),
                (cnt_hbm, cnt_ref),
                (self_hbm, own),
                (weight_hbm, weight),
            )
        )
    ]
    for load in loads:
        load.start()

    barrier = pltpu.get_barrier_semaphore()

    def greet(peer, carry):
        pl.semaphore_signal(barrier, inc=1, device_id={"shard": peer})
        return carry

    lax.fori_loop(me + 1, n, greet, 0)
    for other in range(1, reps):

        @pl.when(other > rep)
        def _():
            pl.semaphore_signal(barrier, inc=1, device_id={"rep": other})

    @pl.when(me + rep > 0)
    def _():
        pl.semaphore_wait(barrier, me + rep)

    def tell(peer, carry):
        pl.semaphore_signal(present.at[me], inc=1, device_id={"shard": peer})
        return carry

    lax.fori_loop(0, me, tell, 0)
    for other in range(reps - 1):

        @pl.when(other < rep)
        def _():
            pl.semaphore_signal(rep_present.at[rep], inc=1, device_id={"rep": other})

    loads[0].wait()
    lists = jnp.concatenate([req_ref[...], jnp.zeros((n, LANES - cap), jnp.int32)], axis=1)
    table[...] = lists.reshape(n, 1, LANES)
    req_recv[me] = table[me]

    loads[3].wait()
    loads[4].wait()

    def ask_copy(peer):
        return pltpu.make_async_remote_copy(
            src_ref=table.at[peer],
            dst_ref=req_recv.at[me],
            send_sem=ask_sem.at[peer],
            recv_sem=ask_recv_sem.at[me],
            device_id={"shard": peer},
        )

    def ask(own_block, to_block):
        for spot in (*range(1, quarter, 2), *range(0, quarter, 2)):
            peer = to_block * quarter + spot
            if to_block > own_block:
                pl.semaphore_wait(present.at[peer], 1)
            if to_block != own_block:
                ask_copy(peer).start()
                continue

            @pl.when(spot > place)
            def _():
                pl.semaphore_wait(present.at[peer], 1)

            @pl.when(spot != place)
            def _():
                ask_copy(peer).start()

    def code_copies():
        peer = POOL * quarter + place
        return [
            pltpu.make_async_remote_copy(
                src_ref=src,
                dst_ref=dst,
                send_sem=code_send_sem.at[i],
                recv_sem=code_recv_sem.at[i],
                device_id={"shard": peer},
            )
            for i, (src, dst) in enumerate(((nbr_ref, pool_codes), (cnt_ref, pool_counts)))
        ]

    def send_codes():
        for copy in code_copies():
            copy.start()

    for b in range(1, 4):

        @pl.when(block == b)
        def _():
            for to_block in range(b):
                ask(b, to_block)

    loads[1].wait()
    high, low = halves(feat[...])
    row_iota = lax.broadcasted_iota(jnp.int32, (LANES, rows), 1)

    loads[2].wait()
    hub_columns = columns_of(jnp.broadcast_to(hub_ref[...], (8, hub_dev)))
    pick = (hub_columns[:, 0:1] == row_iota).astype(jnp.float32).astype(jnp.bfloat16)
    hubs[rep] = dot(pick, high) + dot(pick, low)

    def share_copy(other):
        return pltpu.make_async_remote_copy(
            src_ref=hubs.at[rep],
            dst_ref=hubs.at[rep],
            send_sem=hub_send_sem.at[other],
            recv_sem=hub_recv_sem.at[rep],
            device_id={"rep": other},
        )

    def share():
        for other in range(reps):

            @pl.when(other > rep)
            def _():
                pl.semaphore_wait(rep_present.at[other], 1)

            @pl.when(other != rep)
            def _():
                share_copy(other).start()

    batch = min(LANES // cap, quarter)

    def reply_copy(peer):
        return pltpu.make_async_remote_copy(
            src_ref=gathered.at[peer],
            dst_ref=fetched.at[me],
            send_sem=row_send_sem.at[peer],
            recv_sem=row_recv_sem.at[me],
            device_id={"shard": peer},
        )

    def answer(own_block, peer_block, places):
        peers = [peer_block * quarter + spot for spot in places]

        def unless_me(peer, action):
            if peer_block == own_block:
                pl.when(peer != me)(action)
            else:
                action()

        for peer in peers:
            ref = req_recv.at[peer]
            unless_me(peer, pltpu.make_async_copy(ref, ref, ask_recv_sem.at[peer]).wait)
        request_columns = columns_of(jnp.concatenate([req_recv[peer] for peer in peers], axis=0))
        for first in range(0, len(peers), batch):
            group = peers[first : first + batch]
            pick = jnp.concatenate(
                [
                    (request_columns[:cap, i : i + 1] == row_iota[:cap]).astype(jnp.float32)
                    for i in range(first, first + len(group))
                ],
                axis=0,
            ).astype(jnp.bfloat16)
            picked = dot(pick, high) + dot(pick, low)
            for i, peer in enumerate(group):
                gathered[peer] = picked[i * cap : (i + 1) * cap]
            for peer in group:
                if own_block in (POOL, FEED) and pooled(peer, quarter):
                    row = place + (quarter if own_block == FEED else 0)
                    forward = pltpu.make_async_remote_copy(
                        src_ref=gathered.at[peer],
                        dst_ref=pool.at[row],
                        send_sem=row_send_sem.at[peer],
                        recv_sem=pool_sem.at[row],
                        device_id={"shard": peer + (POOL - CLIENT) * quarter},
                    )
                    if own_block == POOL:
                        pl.when(peer + (POOL - CLIENT) * quarter != me)(forward.start)
                    else:
                        forward.start()
                else:
                    unless_me(peer, reply_copy(peer).start)

    def tally_of(codes, low, count):
        code_iota = low + lax.broadcasted_iota(jnp.int32, (seeds, count), 1)
        tally = jnp.zeros((seeds, count), jnp.float32)
        for k in range(fanout):
            tally = tally + (codes[:, k : k + 1] == code_iota).astype(jnp.float32)
        return tally

    def live_of(counts, low, count):
        spread = (
            low // cap + lax.broadcasted_iota(jnp.int32, (n, count), 1) // cap
            == lax.broadcasted_iota(jnp.int32, (n, count), 0)
        ).astype(jnp.float32).astype(jnp.bfloat16)
        fill = jnp.broadcast_to(counts.astype(jnp.float32), (8, n)).astype(jnp.bfloat16)
        slot_iota = (lax.broadcasted_iota(jnp.int32, (1, count), 1) % cap).astype(jnp.float32)
        return (slot_iota < dot(fill, spread)[0:1]).astype(jnp.float32)

    partial_copy = pltpu.make_async_remote_copy(
        src_ref=partial,
        dst_ref=partial_in,
        send_sem=partial_sem.at[0],
        recv_sem=partial_sem.at[1],
        device_id={"shard": CLIENT * quarter + place},
    )

    def pool_rows():
        for i, ref in enumerate((pool_codes, pool_counts)):
            pltpu.make_async_copy(ref, ref, code_recv_sem.at[i]).wait()
        low = POOL * quarter * cap
        part = quarter * cap
        counted = tally_of(columns_of(pool_codes[...]), hub_total + low, 2 * part)
        counted = (counted * live_of(pool_counts[...], low, 2 * part)).astype(jnp.bfloat16)
        pool[place] = gathered[CLIENT * quarter + place]
        total = None
        for i in range(2):
            for spot in range(quarter):
                row = i * quarter + spot
                arrival = pltpu.make_async_copy(pool.at[row], pool.at[row], pool_sem.at[row])
                if i == 0:
                    pl.when(spot != place)(arrival.wait)
                else:
                    arrival.wait()
            row_high, row_low = halves(pool[i * quarter : (i + 1) * quarter].reshape(part, width))
            chosen = counted[:, i * part : (i + 1) * part]
            term = dot(chosen, row_high) + dot(chosen, row_low)
            total = term if total is None else total + term
        partial[...] = total
        partial_copy.start()

    every, odd, even = range(quarter), range(1, quarter, 2), range(0, quarter, 2)
    front, back = range(quarter // 2), range(quarter // 2, quarter)
    @pl.when(block == 0)
    def _():
        ask(0, 0)
        ask(0, 1)
        ask(0, 2)
        ask(0, 3)
        share()
        answer(0, 1, odd)
        answer(0, 0, every)
        answer(0, 1, even)
        answer(0, 2, every)
        answer(0, 3, every)

    @pl.when(block == 1)
    def _():
        share()
        ask(1, 1)
        ask(1, 2)
        pl.when(lax.rem(me, 2) == 0)(send_codes)
        ask(1, 3)
        answer(1, 2, odd)
        answer(1, 0, every)
        answer(1, 2, even)
        answer(1, 3, every)
        answer(1, 1, every)

    @pl.when(block == 2)
    def _():
        ask(2, 2)
        ask(2, 3)
        share()
        answer(2, 1, odd)
        answer(2, 1, even)
        answer(2, 0, every)
        answer(2, 2, every)
        answer(2, 3, every)
        pl.when(lax.rem(me, 2) == 0)(pool_rows)

    @pl.when(block == 3)
    def _():
        share()
        ask(3, 3)
        answer(3, 3, every)
        answer(3, 1, even)
        answer(3, 2, odd)
        answer(3, 0, every)
        answer(3, 1, odd)
        answer(3, 2, even)

    fetched[me] = gathered[me]

    tally = tally_of(columns_of(nbr_ref[...]), 0, hub_total + n * cap)
    slot_live = live_of(cnt_ref[...], 0, n * cap)
    hub_tally = tally[:, :hub_total]
    live_tally = tally[:, hub_total:] * slot_live
    taken = 1.0 + jnp.sum(hub_tally, axis=1, keepdims=True) + jnp.sum(live_tally, axis=1, keepdims=True)
    scale = 1.0 / taken
    hub_tally = hub_tally.astype(jnp.bfloat16)
    for b in range(4):
        slot_tally[b] = live_tally[:, b * quarter * cap : (b + 1) * quarter * cap].astype(jnp.bfloat16)

    loads[5].wait()
    for other in range(reps):

        @pl.when(other != rep)
        def _():
            pltpu.make_async_copy(hubs.at[other], hubs.at[other], hub_recv_sem.at[other]).wait()

    hub_high, hub_low = halves(hubs[...].reshape(hub_total, width))
    total = own[...] + (dot(hub_tally, hub_high) + dot(hub_tally, hub_low))
    loads[6].wait()
    weight_high, weight_low = halves(weight[...])

    def add_rows(total, owner_block):
        for spot in range(quarter):
            owner = owner_block * quarter + spot

            @pl.when(owner != me)
            def _():
                pltpu.make_async_copy(fetched.at[owner], fetched.at[owner], row_recv_sem.at[owner]).wait()

        row_high, row_low = halves(fetched[pl.ds(owner_block * quarter, quarter)].reshape(quarter * cap, width))
        counted = slot_tally[owner_block]
        return total + (dot(counted, row_high) + dot(counted, row_low))

    def project(total):
        mean_high, mean_low = halves(total * scale)
        out_ref[...] = dot(mean_high, weight_high) + (dot(mean_high, weight_low) + dot(mean_low, weight_high))

    for owner_block in (block, block + 1 - 2 * lax.rem(block, 2)):
        total = add_rows(total, owner_block)
    own[...] = total

    is_client = (block == CLIENT) & (lax.rem(me, 2) == 0)
    is_pool = (block == POOL) & (lax.rem(me, 2) == 0)

    @pl.when(is_client)
    def _():
        pltpu.make_async_copy(partial_in, partial_in, partial_sem.at[1]).wait()
        project(own[...] + partial_in[...])
        for copy in code_copies():
            copy.wait_send()

    @pl.when(jnp.logical_not(is_client))
    def _():
        total = own[...]
        for owner_block in (2 - block // 2, 3 - 3 * (block // 2)):
            total = add_rows(total, owner_block)
        project(total)

    @pl.when(is_pool)
    def _():
        partial_copy.wait_send()

    for peer in range(n):

        @pl.when(peer != me)
        def _():
            ask_copy(peer).wait_send()

        kept = peer + (POOL - CLIENT) * quarter if pooled(peer, quarter) else peer

        @pl.when((peer != me) & (kept != me))
        def _():
            reply_copy(peer).wait_send()

    for other in range(reps):

        @pl.when(other != rep)
        def _():
            share_copy(other).wait_send()


def local(n, reps, features, seed_self, hub_ids, requests, counts, neighbors, weight, out_bias):
    rows, width = features.shape
    cap = requests.shape[1]
    hub_dev = hub_ids.shape[0]
    seeds, fanout = neighbors.shape
    quarter = n // 4
    hbm = pl.BlockSpec(memory_space=pltpu.HBM)
    dma = pltpu.SemaphoreType.DMA
    product = pl.pallas_call(
        functools.partial(kernel, n, reps),
        out_shape=pltpu.VMEM((seeds, width), jnp.float32),
        in_specs=[hbm] * 7,
        out_specs=pl.BlockSpec(memory_space=pltpu.VMEM),
        scratch_shapes=[
            pltpu.VMEM((rows, width), jnp.float32),
            pltpu.VMEM((seeds, width), jnp.float32),
            pltpu.VMEM(weight.shape, jnp.float32),
            pltpu.VMEM((1, hub_dev), jnp.int32),
            pltpu.VMEM((n, cap), jnp.int32),
            pltpu.VMEM((1, n), jnp.int32),
            pltpu.VMEM((fanout, seeds), jnp.int32),
            pltpu.VMEM((n, 1, LANES), jnp.int32),
            pltpu.VMEM((n, 1, LANES), jnp.int32),
            pltpu.VMEM((n, cap, width), jnp.float32),
            pltpu.VMEM((n, cap, width), jnp.float32),
            pltpu.VMEM((reps, hub_dev, width), jnp.float32),
            pltpu.VMEM((4, seeds, quarter * cap), jnp.bfloat16),
            pltpu.VMEM((2 * quarter, cap, width), jnp.float32),
            pltpu.VMEM((fanout, seeds), jnp.int32),
            pltpu.VMEM((1, n), jnp.int32),
            pltpu.VMEM((seeds, width), jnp.float32),
            pltpu.VMEM((seeds, width), jnp.float32),
            dma((7,)),
            dma((n,)),
            dma((n,)),
            dma((n,)),
            dma((n,)),
            dma((reps,)),
            dma((reps,)),
            pltpu.SemaphoreType.REGULAR((n,)),
            pltpu.SemaphoreType.REGULAR((reps,)),
            dma((2 * quarter,)),
            dma((2,)),
            dma((2,)),
            dma((2,)),
        ],
        compiler_params=pltpu.CompilerParams(collective_id=0, has_side_effects=True),
    )(features, seed_self, hub_ids[None], requests, counts[None], neighbors.T, weight)
    return jnp.maximum(product + out_bias, 0.0)


def solution(mesh):
    return jax.shard_map(
        functools.partial(local, mesh.shape["shard"], mesh.shape["rep"]),
        mesh=mesh,
        in_specs=(
            P(("rep", "shard"), None),
            P(("rep", "shard"), None),
            P(("rep", "shard")),
            P(("rep", "shard"), None),
            P(("rep", "shard")),
            P(("rep", "shard"), None),
            P(),
            P(),
        ),
        out_specs=P(("rep", "shard"), None),
        check_vma=False,
    )
```

```python
import functools

import jax
import jax.numpy as jnp
from jax import lax
from jax.experimental import pallas as pl
from jax.experimental.pallas import tpu as pltpu
from jax.sharding import PartitionSpec as P

LANES = 128


def pool_of(peer, quarter):
    block = peer // quarter
    if block in (1, 2) and peer % 2 == 0:
        return peer + (3 - 2 * block) * quarter
    return None


def halves(values):
    high = values.astype(jnp.bfloat16)
    low = (values - high.astype(jnp.float32)).astype(jnp.bfloat16)
    return high, low


def dot(left, right):
    return jnp.dot(left, right, preferred_element_type=jnp.float32)


def columns_of(rows):
    count = rows.shape[0]
    if count < LANES:
        rows = jnp.concatenate([rows, jnp.zeros((LANES - count, LANES), rows.dtype)], axis=0)
    return rows.T


def kernel(
    n, reps, feat_hbm, self_hbm, hub_hbm, req_hbm, cnt_hbm, nbr_hbm, weight_hbm, out_ref,
    feat, own, weight, hub_ref, req_ref, cnt_ref, nbr_ref, table, req_recv, high_ref, low_ref, gathered, fetched, hubs, slot_tally,
    pool, pool_codes, pool_counts, partial, partial_in,
    local_sem, ask_sem, ask_recv_sem, row_send_sem, row_recv_sem, hub_send_sem, hub_recv_sem,
    pool_sem, code_send_sem, code_recv_sem, partial_sem,
):
    me = lax.axis_index("shard")
    rep = lax.axis_index("rep")
    rows, width = feat.shape
    cap = req_ref.shape[1]
    hub_dev = hub_ref.shape[1]
    fanout, seeds = nbr_ref.shape
    hub_total = hub_dev * reps
    quarter = n // 4
    block, place = me // quarter, lax.rem(me, quarter)

    barrier = pltpu.get_barrier_semaphore()
    for off in range(1, n):
        pl.semaphore_signal(barrier, inc=1, device_id={"shard": lax.rem(me + off, n)})
    for off in range(1, reps):
        pl.semaphore_signal(barrier, inc=1, device_id={"rep": lax.rem(rep + off, reps)})

    loads = [
        pltpu.make_async_copy(src, dst, local_sem.at[i])
        for i, (src, dst) in enumerate(
            (
                (req_hbm, req_ref),
                (feat_hbm, feat),
                (hub_hbm, hub_ref),
                (nbr_hbm, nbr_ref),
                (cnt_hbm, cnt_ref),
                (self_hbm, own),
                (weight_hbm, weight),
            )
        )
    ]
    for load in loads:
        load.start()

    loads[0].wait()
    lists = jnp.concatenate([req_ref[...], jnp.zeros((n, LANES - cap), jnp.int32)], axis=1)
    table[...] = lists.reshape(n, 1, LANES)
    req_recv[me] = table[me]

    row_iota = lax.broadcasted_iota(jnp.int32, (LANES, rows), 1)

    def split():
        loads[1].wait()
        high_ref[...], low_ref[...] = halves(feat[...])

    def gather(pick):
        pick = pick.astype(jnp.float32).astype(jnp.bfloat16)
        return dot(pick, high_ref[...]) + dot(pick, low_ref[...])

    def gather_hubs():
        loads[2].wait()
        hub_columns = columns_of(jnp.broadcast_to(hub_ref[...], (8, hub_dev)))
        hubs[rep] = gather(hub_columns[:, 0:1] == row_iota)

    def enter():
        pl.semaphore_wait(barrier, n - 1 + reps - 1)

    loads[3].wait()
    loads[4].wait()

    def ask_copy(peer):
        return pltpu.make_async_remote_copy(
            src_ref=table.at[peer],
            dst_ref=req_recv.at[me],
            send_sem=ask_sem.at[peer],
            recv_sem=ask_recv_sem.at[me],
            device_id={"shard": peer},
        )

    def ask(own_block, to_block):
        for spot in (*range(1, quarter, 2), *range(0, quarter, 2)):
            peer = to_block * quarter + spot
            if to_block != own_block:
                ask_copy(peer).start()
                continue

            @pl.when(spot != place)
            def _():
                ask_copy(peer).start()

    def code_copies():
        peer = (3 - block) * quarter + place
        return [
            pltpu.make_async_remote_copy(
                src_ref=src,
                dst_ref=dst,
                send_sem=code_send_sem.at[i],
                recv_sem=code_recv_sem.at[i],
                device_id={"shard": peer},
            )
            for i, (src, dst) in enumerate(((nbr_ref, pool_codes), (cnt_ref, pool_counts)))
        ]

    def send_codes():
        for copy in code_copies():
            copy.start()

    def share_copy(other):
        return pltpu.make_async_remote_copy(
            src_ref=hubs.at[rep],
            dst_ref=hubs.at[rep],
            send_sem=hub_send_sem.at[other],
            recv_sem=hub_recv_sem.at[rep],
            device_id={"rep": other},
        )

    def share():
        for other in range(reps):

            @pl.when(other != rep)
            def _():
                share_copy(other).start()

    batch = min(LANES // cap, quarter)

    def reply_copy(peer):
        return pltpu.make_async_remote_copy(
            src_ref=gathered.at[peer],
            dst_ref=fetched.at[me],
            send_sem=row_send_sem.at[peer],
            recv_sem=row_recv_sem.at[me],
            device_id={"shard": peer},
        )

    def answer(own_block, peer_block, places):
        peers = [peer_block * quarter + spot for spot in places]

        def unless_me(peer, action):
            if peer_block == own_block:
                pl.when(peer != me)(action)
            else:
                action()

        for peer in peers:
            ref = req_recv.at[peer]
            unless_me(peer, pltpu.make_async_copy(ref, ref, ask_recv_sem.at[peer]).wait)
        request_columns = columns_of(jnp.concatenate([req_recv[peer] for peer in peers], axis=0))
        for first in range(0, len(peers), batch):
            group = peers[first : first + batch]
            picked = gather(
                jnp.concatenate(
                    [
                        request_columns[:cap, i : i + 1] == row_iota[:cap]
                        for i in range(first, first + len(group))
                    ],
                    axis=0,
                )
            )
            for i, peer in enumerate(group):
                gathered[peer] = picked[i * cap : (i + 1) * cap]
            for peer in group:
                pool_peer = pool_of(peer, quarter)
                if pool_peer is not None and own_block // 2 != peer_block // 2:
                    row = lax.rem(me, 2 * quarter)
                    forward = pltpu.make_async_remote_copy(
                        src_ref=gathered.at[peer],
                        dst_ref=pool.at[row],
                        send_sem=row_send_sem.at[peer],
                        recv_sem=pool_sem.at[row],
                        device_id={"shard": pool_peer},
                    )
                    if own_block == 3 - peer_block:
                        pl.when(pool_peer != me)(forward.start)
                    else:
                        forward.start()
                else:
                    unless_me(peer, reply_copy(peer).start)

    def tally_of(codes, low, count):
        code_iota = low + lax.broadcasted_iota(jnp.int32, (seeds, count), 1)
        tally = jnp.zeros((seeds, count), jnp.float32)
        for k in range(fanout):
            tally = tally + (codes[:, k : k + 1] == code_iota).astype(jnp.float32)
        return tally

    def live_of(counts, low, count):
        spread = (
            low // cap + lax.broadcasted_iota(jnp.int32, (n, count), 1) // cap
            == lax.broadcasted_iota(jnp.int32, (n, count), 0)
        ).astype(jnp.float32).astype(jnp.bfloat16)
        fill = jnp.broadcast_to(counts.astype(jnp.float32), (8, n)).astype(jnp.bfloat16)
        slot_iota = (lax.broadcasted_iota(jnp.int32, (1, count), 1) % cap).astype(jnp.float32)
        return (slot_iota < dot(fill, spread)[0:1]).astype(jnp.float32)

    partial_copy = pltpu.make_async_remote_copy(
        src_ref=partial,
        dst_ref=partial_in,
        send_sem=partial_sem.at[0],
        recv_sem=partial_sem.at[1],
        device_id={"shard": (3 - block) * quarter + place},
    )

    def pool_rows(own_block):
        for i, ref in enumerate((pool_codes, pool_counts)):
            pltpu.make_async_copy(ref, ref, code_recv_sem.at[i]).wait()
        low = own_block // 2 * 2 * quarter * cap
        part = quarter * cap
        counted = tally_of(columns_of(pool_codes[...]), hub_total + low, 2 * part)
        counted = (counted * live_of(pool_counts[...], low, 2 * part)).astype(jnp.bfloat16)
        pool[lax.rem(me, 2 * quarter)] = gathered[(3 - own_block) * quarter + place]
        total = None
        own_part = own_block % 2
        for i in (own_part, 1 - own_part):
            for spot in range(quarter):
                row = i * quarter + spot
                arrival = pltpu.make_async_copy(pool.at[row], pool.at[row], pool_sem.at[row])
                if i == own_part:
                    pl.when(spot != place)(arrival.wait)
                else:
                    arrival.wait()
            row_high, row_low = halves(pool[i * quarter : (i + 1) * quarter].reshape(part, width))
            chosen = counted[:, i * part : (i + 1) * part]
            term = dot(chosen, row_high) + dot(chosen, row_low)
            total = term if total is None else total + term
        partial[...] = total
        partial_copy.start()

    every, odd, even = range(quarter), range(1, quarter, 2), range(0, quarter, 2)
    front, back = range(quarter // 2), range(quarter // 2, quarter)
    @pl.when(block == 0)
    def _():
        split()
        gather_hubs()
        enter()
        ask(0, 3)
        ask(0, 2)
        ask(0, 1)
        ask(0, 0)
        share()
        answer(0, 2, even)
        answer(0, 0, every)
        answer(0, 3, every)
        answer(0, 1, every)
        answer(0, 2, odd)

    @pl.when(block == 1)
    def _():
        split()
        gather_hubs()
        enter()
        ask(1, 3)
        ask(1, 0)
        ask(1, 2)
        pl.when(lax.rem(me, 2) == 0)(send_codes)
        ask(1, 1)
        answer(1, 2, odd)
        answer(1, 0, every)
        answer(1, 2, even)
        share()
        answer(1, 3, every)
        answer(1, 1, every)
        pl.when(lax.rem(me, 2) == 0)(functools.partial(pool_rows, 1))

    @pl.when(block == 2)
    def _():
        split()
        enter()
        ask(2, 0)
        ask(2, 1)
        pl.when(lax.rem(me, 2) == 0)(send_codes)
        ask(2, 2)
        ask(2, 3)
        gather_hubs()
        share()
        answer(2, 1, odd)
        answer(2, 1, even)
        answer(2, 0, every)
        answer(2, 2, every)
        answer(2, 3, every)
        pl.when(lax.rem(me, 2) == 0)(functools.partial(pool_rows, 2))

    @pl.when(block == 3)
    def _():
        enter()
        ask(3, 0)
        ask(3, 1)
        ask(3, 2)
        ask(3, 3)
        split()
        gather_hubs()
        answer(3, 3, every)
        answer(3, 1, even)
        answer(3, 1, odd)
        share()
        answer(3, 0, every)
        answer(3, 2, every)

    fetched[me] = gathered[me]

    tally = tally_of(columns_of(nbr_ref[...]), 0, hub_total + n * cap)
    slot_live = live_of(cnt_ref[...], 0, n * cap)
    hub_tally = tally[:, :hub_total]
    live_tally = tally[:, hub_total:] * slot_live
    taken = 1.0 + jnp.sum(hub_tally, axis=1, keepdims=True) + jnp.sum(live_tally, axis=1, keepdims=True)
    scale = 1.0 / taken
    hub_tally = hub_tally.astype(jnp.bfloat16)
    for b in range(4):
        slot_tally[b] = live_tally[:, b * quarter * cap : (b + 1) * quarter * cap].astype(jnp.bfloat16)

    loads[5].wait()
    for other in range(reps):

        @pl.when(other != rep)
        def _():
            pltpu.make_async_copy(hubs.at[other], hubs.at[other], hub_recv_sem.at[other]).wait()

    hub_high, hub_low = halves(hubs[...].reshape(hub_total, width))
    total = own[...] + (dot(hub_tally, hub_high) + dot(hub_tally, hub_low))
    loads[6].wait()
    weight_high, weight_low = halves(weight[...])

    def add_rows(total, owner_block):
        for spot in range(quarter):
            owner = owner_block * quarter + spot

            @pl.when(owner != me)
            def _():
                pltpu.make_async_copy(fetched.at[owner], fetched.at[owner], row_recv_sem.at[owner]).wait()

        row_high, row_low = halves(fetched[pl.ds(owner_block * quarter, quarter)].reshape(quarter * cap, width))
        counted = slot_tally[owner_block]
        return total + (dot(counted, row_high) + dot(counted, row_low))

    def project(total):
        mean_high, mean_low = halves(total * scale)
        out_ref[...] = dot(mean_high, weight_high) + (dot(mean_high, weight_low) + dot(mean_low, weight_high))

    for owner_block in (block, block + 1 - 2 * lax.rem(block, 2)):
        total = add_rows(total, owner_block)
    own[...] = total

    is_client = ((block == 1) | (block == 2)) & (lax.rem(me, 2) == 0)

    @pl.when(is_client)
    def _():
        pltpu.make_async_copy(partial_in, partial_in, partial_sem.at[1]).wait()
        project(own[...] + partial_in[...])
        for copy in (*code_copies(), partial_copy):
            copy.wait_send()

    @pl.when(jnp.logical_not(is_client))
    def _():
        total = own[...]
        for owner_block in (2 - block // 2, 3 - 3 * (block // 2)):
            total = add_rows(total, owner_block)
        project(total)

    for peer in range(n):

        @pl.when(peer != me)
        def _():
            ask_copy(peer).wait_send()

        pool_peer = pool_of(peer, quarter)
        kept = peer if pool_peer is None else pool_peer

        @pl.when((peer != me) & (kept != me))
        def _():
            reply_copy(peer).wait_send()

    for other in range(reps):

        @pl.when(other != rep)
        def _():
            share_copy(other).wait_send()


def local(n, reps, features, seed_self, hub_ids, requests, counts, neighbors, weight, out_bias):
    rows, width = features.shape
    cap = requests.shape[1]
    hub_dev = hub_ids.shape[0]
    seeds, fanout = neighbors.shape
    quarter = n // 4
    hbm = pl.BlockSpec(memory_space=pltpu.HBM)
    dma = pltpu.SemaphoreType.DMA
    product = pl.pallas_call(
        functools.partial(kernel, n, reps),
        out_shape=pltpu.VMEM((seeds, width), jnp.float32),
        in_specs=[hbm] * 7,
        out_specs=pl.BlockSpec(memory_space=pltpu.VMEM),
        scratch_shapes=[
            pltpu.VMEM((rows, width), jnp.float32),
            pltpu.VMEM((seeds, width), jnp.float32),
            pltpu.VMEM(weight.shape, jnp.float32),
            pltpu.VMEM((1, hub_dev), jnp.int32),
            pltpu.VMEM((n, cap), jnp.int32),
            pltpu.VMEM((1, n), jnp.int32),
            pltpu.VMEM((fanout, seeds), jnp.int32),
            pltpu.VMEM((n, 1, LANES), jnp.int32),
            pltpu.VMEM((n, 1, LANES), jnp.int32),
            pltpu.VMEM((rows, width), jnp.bfloat16),
            pltpu.VMEM((rows, width), jnp.bfloat16),
            pltpu.VMEM((n, cap, width), jnp.float32),
            pltpu.VMEM((n, cap, width), jnp.float32),
            pltpu.VMEM((reps, hub_dev, width), jnp.float32),
            pltpu.VMEM((4, seeds, quarter * cap), jnp.bfloat16),
            pltpu.VMEM((2 * quarter, cap, width), jnp.float32),
            pltpu.VMEM((fanout, seeds), jnp.int32),
            pltpu.VMEM((1, n), jnp.int32),
            pltpu.VMEM((seeds, width), jnp.float32),
            pltpu.VMEM((seeds, width), jnp.float32),
            dma((7,)),
            dma((n,)),
            dma((n,)),
            dma((n,)),
            dma((n,)),
            dma((reps,)),
            dma((reps,)),
            dma((2 * quarter,)),
            dma((2,)),
            dma((2,)),
            dma((2,)),
        ],
        compiler_params=pltpu.CompilerParams(collective_id=0, has_side_effects=True),
    )(features, seed_self, hub_ids[None], requests, counts[None], neighbors.T, weight)
    return jnp.maximum(product + out_bias, 0.0)


def solution(mesh):
    return jax.shard_map(
        functools.partial(local, mesh.shape["shard"], mesh.shape["rep"]),
        mesh=mesh,
        in_specs=(
            P(("rep", "shard"), None),
            P(("rep", "shard"), None),
            P(("rep", "shard")),
            P(("rep", "shard"), None),
            P(("rep", "shard")),
            P(("rep", "shard"), None),
            P(),
            P(),
        ),
        out_specs=P(("rep", "shard"), None),
        check_vma=False,
    )
```

```python
import functools

import jax
import jax.numpy as jnp
from jax import lax
from jax.experimental import pallas as pl
from jax.experimental.pallas import tpu as pltpu
from jax.sharding import PartitionSpec as P

LANES = 128


def pool_of(peer, quarter):
    block = peer // quarter
    if block in (1, 2) and peer % 2 == 0:
        return peer + (3 - 2 * block) * quarter
    return None


def halves(values):
    high = values.astype(jnp.bfloat16)
    low = (values - high.astype(jnp.float32)).astype(jnp.bfloat16)
    return high, low


def dot(left, right):
    return jnp.dot(left, right, preferred_element_type=jnp.float32)


def columns_of(rows):
    count = rows.shape[0]
    if count < LANES:
        rows = jnp.concatenate([rows, jnp.zeros((LANES - count, LANES), rows.dtype)], axis=0)
    return rows.T


def kernel(
    n, reps, feat_hbm, self_hbm, hub_hbm, req_hbm, cnt_hbm, nbr_hbm, weight_hbm, out_ref,
    feat, own, weight, hub_ref, req_ref, cnt_ref, nbr_ref, table, req_recv, high_ref, low_ref, gathered, fetched, hubs, slot_tally,
    pool, pool_codes, pool_counts, partial, partial_in,
    local_sem, ask_recv_sem, row_recv_sem, hub_recv_sem, pool_sem, code_recv_sem, partial_sem,
):
    me = lax.axis_index("shard")
    rep = lax.axis_index("rep")
    rows, width = feat.shape
    cap = req_ref.shape[1]
    hub_dev = hub_ref.shape[1]
    fanout, seeds = nbr_ref.shape
    hub_total = hub_dev * reps
    quarter = n // 4
    block, place = me // quarter, lax.rem(me, quarter)

    barrier = pltpu.get_barrier_semaphore()
    for off in range(1, n):
        pl.semaphore_signal(barrier, inc=1, device_id={"shard": lax.rem(me + off, n)})
    for off in range(1, reps):
        pl.semaphore_signal(barrier, inc=1, device_id={"rep": lax.rem(rep + off, reps)})

    loads = [
        pltpu.make_async_copy(src, dst, local_sem.at[i])
        for i, (src, dst) in enumerate(
            (
                (req_hbm, req_ref),
                (feat_hbm, feat),
                (hub_hbm, hub_ref),
                (nbr_hbm, nbr_ref),
                (cnt_hbm, cnt_ref),
                (self_hbm, own),
                (weight_hbm, weight),
            )
        )
    ]
    for load in loads:
        load.start()

    loads[0].wait()
    lists = jnp.concatenate([req_ref[...], jnp.zeros((n, LANES - cap), jnp.int32)], axis=1)
    table[...] = lists.reshape(n, 1, LANES)
    req_recv[me] = table[me]

    row_iota = lax.broadcasted_iota(jnp.int32, (LANES, rows), 1)

    def split():
        for load in (loads[1], loads[5], loads[6]):
            load.wait()
        high_ref[...], low_ref[...] = halves(feat[...])

    def gather(pick):
        pick = pick.astype(jnp.float32).astype(jnp.bfloat16)
        return dot(pick, high_ref[...]) + dot(pick, low_ref[...])

    def gather_hubs():
        loads[2].wait()
        hub_columns = columns_of(jnp.broadcast_to(hub_ref[...], (8, hub_dev)))
        hubs[rep] = gather(hub_columns[:, 0:1] == row_iota)

    def enter():
        pl.semaphore_wait(barrier, n - 1 + reps - 1)

    loads[3].wait()
    loads[4].wait()

    def ask_copy(peer):
        return pltpu.make_async_remote_copy(
            src_ref=table.at[peer],
            dst_ref=req_recv.at[me],
            send_sem=local_sem.at[0],
            recv_sem=ask_recv_sem.at[2 * block + lax.rem(me, 2)],
            device_id={"shard": peer},
        )

    def ask(own_block, to_block):
        for spot in (*range(1, quarter, 2), *range(0, quarter, 2)):
            peer = to_block * quarter + spot
            if to_block != own_block:
                ask_copy(peer).start()
                continue

            @pl.when(spot != place)
            def _():
                ask_copy(peer).start()

    def code_copies():
        peer = (3 - block) * quarter + place
        return [
            pltpu.make_async_remote_copy(
                src_ref=src,
                dst_ref=dst,
                send_sem=local_sem.at[3 + i],
                recv_sem=code_recv_sem.at[i],
                device_id={"shard": peer},
            )
            for i, (src, dst) in enumerate(((nbr_ref, pool_codes), (cnt_ref, pool_counts)))
        ]

    def send_codes():
        for copy in code_copies():
            copy.start()

    def share_copy(other):
        return pltpu.make_async_remote_copy(
            src_ref=hubs.at[rep],
            dst_ref=hubs.at[rep],
            send_sem=local_sem.at[2],
            recv_sem=hub_recv_sem.at[0],
            device_id={"rep": other},
        )

    def share():
        for other in range(reps):

            @pl.when(other != rep)
            def _():
                share_copy(other).start()

    def take(buffer, count, sem):
        part = buffer.at[pl.ds(0, count)]
        pltpu.make_async_copy(part, part, sem).wait()

    batch = min(LANES // cap, quarter)

    def reply_copy(peer):
        return pltpu.make_async_remote_copy(
            src_ref=gathered.at[peer],
            dst_ref=fetched.at[me],
            send_sem=local_sem.at[1],
            recv_sem=row_recv_sem.at[block],
            device_id={"shard": peer},
        )

    def answer(own_block, peer_block, places):
        peers = [peer_block * quarter + spot for spot in places]

        def unless_me(peer, action):
            if peer_block == own_block:
                pl.when(peer != me)(action)
            else:
                action()

        for parity in sorted({spot % 2 for spot in places}):
            sem = ask_recv_sem.at[2 * peer_block + parity]
            count = quarter // 2
            if peer_block != own_block:
                take(req_recv, count, sem)
                continue

            @pl.when(lax.rem(me, 2) == parity)
            def _():
                take(req_recv, count - 1, sem)

            @pl.when(lax.rem(me, 2) != parity)
            def _():
                take(req_recv, count, sem)

        request_columns = columns_of(jnp.concatenate([req_recv[peer] for peer in peers], axis=0))
        for first in range(0, len(peers), batch):
            group = peers[first : first + batch]
            picked = gather(
                jnp.concatenate(
                    [
                        request_columns[:cap, i : i + 1] == row_iota[:cap]
                        for i in range(first, first + len(group))
                    ],
                    axis=0,
                )
            )
            for i, peer in enumerate(group):
                gathered[peer] = picked[i * cap : (i + 1) * cap]
            for peer in group:
                pool_peer = pool_of(peer, quarter)
                if pool_peer is not None and own_block // 2 != peer_block // 2:
                    row = lax.rem(me, 2 * quarter)
                    forward = pltpu.make_async_remote_copy(
                        src_ref=gathered.at[peer],
                        dst_ref=pool.at[row],
                        send_sem=local_sem.at[1],
                        recv_sem=pool_sem.at[lax.rem(block, 2)],
                        device_id={"shard": pool_peer},
                    )
                    if own_block == 3 - peer_block:
                        pl.when(pool_peer != me)(forward.start)
                    else:
                        forward.start()
                else:
                    unless_me(peer, reply_copy(peer).start)

    def tally_of(codes, low, count):
        code_iota = low + lax.broadcasted_iota(jnp.int32, (seeds, count), 1)
        tally = jnp.zeros((seeds, count), jnp.float32)
        for k in range(fanout):
            tally = tally + (codes[:, k : k + 1] == code_iota).astype(jnp.float32)
        return tally

    def live_of(counts, low, count):
        spread = (
            low // cap + lax.broadcasted_iota(jnp.int32, (n, count), 1) // cap
            == lax.broadcasted_iota(jnp.int32, (n, count), 0)
        ).astype(jnp.float32).astype(jnp.bfloat16)
        fill = jnp.broadcast_to(counts.astype(jnp.float32), (8, n)).astype(jnp.bfloat16)
        slot_iota = (lax.broadcasted_iota(jnp.int32, (1, count), 1) % cap).astype(jnp.float32)
        return (slot_iota < dot(fill, spread)[0:1]).astype(jnp.float32)

    partial_copy = pltpu.make_async_remote_copy(
        src_ref=partial,
        dst_ref=partial_in,
        send_sem=local_sem.at[5],
        recv_sem=partial_sem.at[0],
        device_id={"shard": (3 - block) * quarter + place},
    )

    def pool_rows(own_block):
        for i, ref in enumerate((pool_codes, pool_counts)):
            pltpu.make_async_copy(ref, ref, code_recv_sem.at[i]).wait()
        low = own_block // 2 * 2 * quarter * cap
        part = quarter * cap
        counted = tally_of(columns_of(pool_codes[...]), hub_total + low, 2 * part)
        counted = (counted * live_of(pool_counts[...], low, 2 * part)).astype(jnp.bfloat16)
        pool[lax.rem(me, 2 * quarter)] = gathered[(3 - own_block) * quarter + place]
        total = None
        own_part = own_block % 2
        for i in (own_part, 1 - own_part):
            take(pool, quarter - 1 if i == own_part else quarter, pool_sem.at[i])
            row_high, row_low = halves(pool[i * quarter : (i + 1) * quarter].reshape(part, width))
            chosen = counted[:, i * part : (i + 1) * part]
            term = dot(chosen, row_high) + dot(chosen, row_low)
            total = term if total is None else total + term
        partial[...] = total
        partial_copy.start()

    every, odd, even = range(quarter), range(1, quarter, 2), range(0, quarter, 2)
    front, back = range(quarter // 2), range(quarter // 2, quarter)
    @pl.when(block == 0)
    def _():
        split()
        gather_hubs()
        enter()
        ask(0, 3)
        ask(0, 2)
        ask(0, 1)
        ask(0, 0)
        share()
        answer(0, 2, even)
        answer(0, 0, every)
        answer(0, 3, every)
        answer(0, 1, every)
        answer(0, 2, odd)

    @pl.when(block == 1)
    def _():
        split()
        gather_hubs()
        enter()
        ask(1, 3)
        ask(1, 0)
        ask(1, 2)
        pl.when(lax.rem(me, 2) == 0)(send_codes)
        ask(1, 1)
        answer(1, 2, odd)
        answer(1, 0, every)
        answer(1, 2, even)
        share()
        answer(1, 3, every)
        answer(1, 1, every)
        pl.when(lax.rem(me, 2) == 0)(functools.partial(pool_rows, 1))

    @pl.when(block == 2)
    def _():
        split()
        enter()
        ask(2, 0)
        ask(2, 1)
        pl.when(lax.rem(me, 2) == 0)(send_codes)
        ask(2, 2)
        ask(2, 3)
        gather_hubs()
        share()
        answer(2, 1, odd)
        answer(2, 1, even)
        answer(2, 0, every)
        answer(2, 2, every)
        answer(2, 3, every)
        pl.when(lax.rem(me, 2) == 0)(functools.partial(pool_rows, 2))

    @pl.when(block == 3)
    def _():
        enter()
        ask(3, 0)
        ask(3, 1)
        ask(3, 2)
        ask(3, 3)
        split()
        gather_hubs()
        answer(3, 3, every)
        answer(3, 1, even)
        answer(3, 1, odd)
        share()
        answer(3, 0, every)
        answer(3, 2, every)

    fetched[me] = gathered[me]

    tally = tally_of(columns_of(nbr_ref[...]), 0, hub_total + n * cap)
    slot_live = live_of(cnt_ref[...], 0, n * cap)
    hub_tally = tally[:, :hub_total]
    live_tally = tally[:, hub_total:] * slot_live
    taken = 1.0 + jnp.sum(hub_tally, axis=1, keepdims=True) + jnp.sum(live_tally, axis=1, keepdims=True)
    scale = 1.0 / taken
    hub_tally = hub_tally.astype(jnp.bfloat16)
    for b in range(4):
        slot_tally[b] = live_tally[:, b * quarter * cap : (b + 1) * quarter * cap].astype(jnp.bfloat16)

    take(table, n - 1, local_sem.at[0])
    if reps > 1:
        take(hubs, reps - 1, local_sem.at[2])
        take(hubs, reps - 1, hub_recv_sem.at[0])
    hub_high, hub_low = halves(hubs[...].reshape(hub_total, width))
    total = own[...] + (dot(hub_tally, hub_high) + dot(hub_tally, hub_low))
    weight_high, weight_low = halves(weight[...])

    def add_rows(total, owner_block, count):
        take(fetched, count, row_recv_sem.at[owner_block])
        row_high, row_low = halves(fetched[pl.ds(owner_block * quarter, quarter)].reshape(quarter * cap, width))
        counted = slot_tally[owner_block]
        return total + (dot(counted, row_high) + dot(counted, row_low))

    def project(total):
        mean_high, mean_low = halves(total * scale)
        out_ref[...] = dot(mean_high, weight_high) + (dot(mean_high, weight_low) + dot(mean_low, weight_high))

    total = add_rows(total, block, quarter - 1)
    own[...] = add_rows(total, block + 1 - 2 * lax.rem(block, 2), quarter)

    is_client = ((block == 1) | (block == 2)) & (lax.rem(me, 2) == 0)

    @pl.when(is_client)
    def _():
        take(gathered, n - 2, local_sem.at[1])
        for copy in (*code_copies(), partial_copy):
            copy.wait_send()
        pltpu.make_async_copy(partial_in, partial_in, partial_sem.at[0]).wait()
        project(own[...] + partial_in[...])

    @pl.when(jnp.logical_not(is_client))
    def _():
        take(gathered, n - 1, local_sem.at[1])
        total = own[...]
        for owner_block in (2 - block // 2, 3 - 3 * (block // 2)):
            total = add_rows(total, owner_block, quarter)
        project(total)


def local(n, reps, features, seed_self, hub_ids, requests, counts, neighbors, weight, out_bias):
    rows, width = features.shape
    cap = requests.shape[1]
    hub_dev = hub_ids.shape[0]
    seeds, fanout = neighbors.shape
    quarter = n // 4
    hbm = pl.BlockSpec(memory_space=pltpu.HBM)
    dma = pltpu.SemaphoreType.DMA
    product = pl.pallas_call(
        functools.partial(kernel, n, reps),
        out_shape=pltpu.VMEM((seeds, width), jnp.float32),
        in_specs=[hbm] * 7,
        out_specs=pl.BlockSpec(memory_space=pltpu.VMEM),
        scratch_shapes=[
            pltpu.VMEM((rows, width), jnp.float32),
            pltpu.VMEM((seeds, width), jnp.float32),
            pltpu.VMEM(weight.shape, jnp.float32),
            pltpu.VMEM((1, hub_dev), jnp.int32),
            pltpu.VMEM((n, cap), jnp.int32),
            pltpu.VMEM((1, n), jnp.int32),
            pltpu.VMEM((fanout, seeds), jnp.int32),
            pltpu.VMEM((n, 1, LANES), jnp.int32),
            pltpu.VMEM((n, 1, LANES), jnp.int32),
            pltpu.VMEM((rows, width), jnp.bfloat16),
            pltpu.VMEM((rows, width), jnp.bfloat16),
            pltpu.VMEM((n, cap, width), jnp.float32),
            pltpu.VMEM((n, cap, width), jnp.float32),
            pltpu.VMEM((reps, hub_dev, width), jnp.float32),
            pltpu.VMEM((4, seeds, quarter * cap), jnp.bfloat16),
            pltpu.VMEM((2 * quarter, cap, width), jnp.float32),
            pltpu.VMEM((fanout, seeds), jnp.int32),
            pltpu.VMEM((1, n), jnp.int32),
            pltpu.VMEM((seeds, width), jnp.float32),
            pltpu.VMEM((seeds, width), jnp.float32),
            dma((7,)),
            dma((8,)),
            dma((4,)),
            dma((1,)),
            dma((2,)),
            dma((2,)),
            dma((1,)),
        ],
        compiler_params=pltpu.CompilerParams(collective_id=0, has_side_effects=True),
    )(features, seed_self, hub_ids[None], requests, counts[None], neighbors.T, weight)
    return jnp.maximum(product + out_bias, 0.0)


def solution(mesh):
    return jax.shard_map(
        functools.partial(local, mesh.shape["shard"], mesh.shape["rep"]),
        mesh=mesh,
        in_specs=(
            P(("rep", "shard"), None),
            P(("rep", "shard"), None),
            P(("rep", "shard")),
            P(("rep", "shard"), None),
            P(("rep", "shard")),
            P(("rep", "shard"), None),
            P(),
            P(),
        ),
        out_specs=P(("rep", "shard"), None),
        check_vma=False,
    )
```

```python
import functools

import jax
import jax.numpy as jnp
from jax import lax
from jax.experimental import pallas as pl
from jax.experimental.pallas import tpu as pltpu
from jax.sharding import PartitionSpec as P

LANES = 128


def pool_of(peer, quarter):
    block = peer // quarter
    if block in (1, 2) and peer % 2 == 0:
        return peer + (3 - 2 * block) * quarter
    return None


def halves(values):
    high = values.astype(jnp.bfloat16)
    low = (values - high.astype(jnp.float32)).astype(jnp.bfloat16)
    return high, low


def dot(left, right):
    return jnp.dot(left, right, preferred_element_type=jnp.float32)


def columns_of(rows):
    count = rows.shape[0]
    if count < LANES:
        rows = jnp.concatenate([rows, jnp.zeros((LANES - count, LANES), rows.dtype)], axis=0)
    return rows.T


def kernel(
    n, reps, feat_hbm, self_hbm, hub_hbm, req_hbm, cnt_hbm, nbr_hbm, weight_hbm, out_ref,
    feat, own, weight, hub_ref, req_ref, cnt_ref, nbr_ref, table, req_recv, high_ref, low_ref, gathered, fetched, hubs, slot_tally,
    pool, pool_codes, pool_counts, partial, partial_in,
    local_sem, ask_recv_sem, row_recv_sem, hub_recv_sem, pool_sem, code_recv_sem, partial_sem,
):
    me = lax.axis_index("shard")
    rep = lax.axis_index("rep")
    rows, width = feat.shape
    cap = req_ref.shape[1]
    hub_dev = hub_ref.shape[1]
    fanout, seeds = nbr_ref.shape
    hub_total = hub_dev * reps
    quarter = n // 4
    block, place = me // quarter, lax.rem(me, quarter)

    barrier = pltpu.get_barrier_semaphore()
    for off in range(1, n):
        pl.semaphore_signal(barrier, inc=1, device_id={"shard": lax.rem(me + off, n)})
    for off in range(1, reps):
        pl.semaphore_signal(barrier, inc=1, device_id={"rep": lax.rem(rep + off, reps)})

    loads = [
        pltpu.make_async_copy(src, dst, local_sem.at[i])
        for i, (src, dst) in enumerate(
            (
                (req_hbm, req_ref),
                (feat_hbm, feat),
                (hub_hbm, hub_ref),
                (nbr_hbm, nbr_ref),
                (cnt_hbm, cnt_ref),
                (self_hbm, own),
                (weight_hbm, weight),
            )
        )
    ]
    for load in loads:
        load.start()

    loads[0].wait()
    lists = jnp.concatenate([req_ref[...], jnp.zeros((n, LANES - cap), jnp.int32)], axis=1)
    table[...] = lists.reshape(n, 1, LANES)
    req_recv[me] = table[me]

    row_iota = lax.broadcasted_iota(jnp.int32, (LANES, rows), 1)

    def split():
        for load in (loads[1], loads[5], loads[6]):
            load.wait()
        high_ref[...], low_ref[...] = halves(feat[...])

    def gather(pick):
        pick = pick.astype(jnp.float32).astype(jnp.bfloat16)
        return dot(pick, high_ref[...]) + dot(pick, low_ref[...])

    def gather_hubs():
        loads[2].wait()
        hub_columns = columns_of(jnp.broadcast_to(hub_ref[...], (8, hub_dev)))
        hubs[rep] = gather(hub_columns[:, 0:1] == row_iota)

    def enter():
        pl.semaphore_wait(barrier, n - 1 + reps - 1)

    loads[3].wait()
    loads[4].wait()

    def ask_copy(peer):
        return pltpu.make_async_remote_copy(
            src_ref=table.at[peer],
            dst_ref=req_recv.at[me],
            send_sem=local_sem.at[0],
            recv_sem=ask_recv_sem.at[2 * block + lax.rem(me, 2)],
            device_id={"shard": peer},
        )

    def ask(own_block, to_block):
        for spot in (*range(1, quarter, 2), *range(0, quarter, 2)):
            peer = to_block * quarter + spot
            if to_block != own_block:
                ask_copy(peer).start()
                continue

            @pl.when(spot != place)
            def _():
                ask_copy(peer).start()

    def code_copies():
        peer = (3 - block) * quarter + place
        return [
            pltpu.make_async_remote_copy(
                src_ref=src,
                dst_ref=dst,
                send_sem=local_sem.at[3 + i],
                recv_sem=code_recv_sem.at[i],
                device_id={"shard": peer},
            )
            for i, (src, dst) in enumerate(((nbr_ref, pool_codes), (cnt_ref, pool_counts)))
        ]

    def send_codes():
        for copy in code_copies():
            copy.start()

    def share_copy(other):
        return pltpu.make_async_remote_copy(
            src_ref=hubs.at[rep],
            dst_ref=hubs.at[rep],
            send_sem=local_sem.at[2],
            recv_sem=hub_recv_sem.at[0],
            device_id={"rep": other},
        )

    def share():
        for other in range(reps):

            @pl.when(other != rep)
            def _():
                share_copy(other).start()

    def take(buffer, count, sem):
        part = buffer.at[pl.ds(0, count)]
        pltpu.make_async_copy(part, part, sem).wait()

    batch = min(LANES // cap, quarter)

    def reply_copy(peer):
        return pltpu.make_async_remote_copy(
            src_ref=gathered.at[peer],
            dst_ref=fetched.at[me],
            send_sem=local_sem.at[1],
            recv_sem=row_recv_sem.at[block],
            device_id={"shard": peer},
        )

    def answer(own_block, peer_block, places):
        peers = [peer_block * quarter + spot for spot in places]

        def unless_me(peer, action):
            if peer_block == own_block:
                pl.when(peer != me)(action)
            else:
                action()

        for parity in sorted({spot % 2 for spot in places}):
            sem = ask_recv_sem.at[2 * peer_block + parity]
            count = quarter // 2
            if peer_block != own_block:
                take(req_recv, count, sem)
                continue

            @pl.when(lax.rem(me, 2) == parity)
            def _():
                take(req_recv, count - 1, sem)

            @pl.when(lax.rem(me, 2) != parity)
            def _():
                take(req_recv, count, sem)

        request_columns = columns_of(jnp.concatenate([req_recv[peer] for peer in peers], axis=0))
        for first in range(0, len(peers), batch):
            group = peers[first : first + batch]
            picked = gather(
                jnp.concatenate(
                    [
                        request_columns[:cap, i : i + 1] == row_iota[:cap]
                        for i in range(first, first + len(group))
                    ],
                    axis=0,
                )
            )
            for i, peer in enumerate(group):
                gathered[peer] = picked[i * cap : (i + 1) * cap]
            for peer in group:
                pool_peer = pool_of(peer, quarter)
                if pool_peer is not None and own_block // 2 != peer_block // 2:
                    row = lax.rem(me, 2 * quarter)
                    forward = pltpu.make_async_remote_copy(
                        src_ref=gathered.at[peer],
                        dst_ref=pool.at[row],
                        send_sem=local_sem.at[1],
                        recv_sem=pool_sem.at[lax.rem(block, 2)],
                        device_id={"shard": pool_peer},
                    )
                    if own_block == 3 - peer_block:
                        pl.when(pool_peer != me)(forward.start)
                    else:
                        forward.start()
                else:
                    unless_me(peer, reply_copy(peer).start)

    def tally_of(codes, low, count):
        code_iota = low + lax.broadcasted_iota(jnp.int32, (seeds, count), 1)
        tally = jnp.zeros((seeds, count), jnp.float32)
        for k in range(fanout):
            tally = tally + (codes[:, k : k + 1] == code_iota).astype(jnp.float32)
        return tally

    def live_of(counts, low, count):
        spread = (
            low // cap + lax.broadcasted_iota(jnp.int32, (n, count), 1) // cap
            == lax.broadcasted_iota(jnp.int32, (n, count), 0)
        ).astype(jnp.float32).astype(jnp.bfloat16)
        fill = jnp.broadcast_to(counts.astype(jnp.float32), (8, n)).astype(jnp.bfloat16)
        slot_iota = (lax.broadcasted_iota(jnp.int32, (1, count), 1) % cap).astype(jnp.float32)
        return (slot_iota < dot(fill, spread)[0:1]).astype(jnp.float32)

    partial_copy = pltpu.make_async_remote_copy(
        src_ref=partial,
        dst_ref=partial_in,
        send_sem=local_sem.at[5],
        recv_sem=partial_sem.at[0],
        device_id={"shard": (3 - block) * quarter + place},
    )

    def pool_rows(own_block):
        for i, ref in enumerate((pool_codes, pool_counts)):
            pltpu.make_async_copy(ref, ref, code_recv_sem.at[i]).wait()
        low = own_block // 2 * 2 * quarter * cap
        part = quarter * cap
        counted = tally_of(columns_of(pool_codes[...]), hub_total + low, 2 * part)
        counted = (counted * live_of(pool_counts[...], low, 2 * part)).astype(jnp.bfloat16)
        pool[lax.rem(me, 2 * quarter)] = gathered[(3 - own_block) * quarter + place]
        total = None
        own_part = own_block % 2
        for i in (own_part, 1 - own_part):
            take(pool, quarter - 1 if i == own_part else quarter, pool_sem.at[i])
            row_high, row_low = halves(pool[i * quarter : (i + 1) * quarter].reshape(part, width))
            chosen = counted[:, i * part : (i + 1) * part]
            term = dot(chosen, row_high) + dot(chosen, row_low)
            total = term if total is None else total + term
        partial[...] = total
        partial_copy.start()

    every, odd, even = range(quarter), range(1, quarter, 2), range(0, quarter, 2)
    front, back = range(quarter // 2), range(quarter // 2, quarter)
    @pl.when(block == 0)
    def _():
        split()
        gather_hubs()
        enter()
        ask(0, 3)
        ask(0, 2)
        ask(0, 1)
        ask(0, 0)
        share()
        answer(0, 2, even)
        answer(0, 0, every)
        answer(0, 3, every)
        answer(0, 1, every)
        answer(0, 2, odd)

    @pl.when(block == 1)
    def _():
        split()
        gather_hubs()
        enter()
        ask(1, 3)
        ask(1, 0)
        ask(1, 2)
        pl.when(lax.rem(me, 2) == 0)(send_codes)
        ask(1, 1)
        answer(1, 2, odd)
        answer(1, 0, every)
        answer(1, 2, even)
        share()
        answer(1, 3, every)
        answer(1, 1, every)
        pl.when(lax.rem(me, 2) == 0)(functools.partial(pool_rows, 1))

    @pl.when(block == 2)
    def _():
        split()
        enter()
        ask(2, 0)
        ask(2, 1)
        pl.when(lax.rem(me, 2) == 0)(send_codes)
        ask(2, 2)
        ask(2, 3)
        gather_hubs()
        share()
        answer(2, 1, odd)
        answer(2, 1, even)
        answer(2, 0, every)
        answer(2, 2, every)
        answer(2, 3, every)
        pl.when(lax.rem(me, 2) == 0)(functools.partial(pool_rows, 2))

    @pl.when(block == 3)
    def _():
        enter()
        ask(3, 0)
        ask(3, 1)
        ask(3, 2)
        ask(3, 3)
        split()
        gather_hubs()
        answer(3, 3, every)
        answer(3, 1, even)
        answer(3, 1, odd)
        share()
        answer(3, 0, every)
        answer(3, 2, every)

    fetched[me] = gathered[me]

    tally = tally_of(columns_of(nbr_ref[...]), 0, hub_total + n * cap)
    slot_live = live_of(cnt_ref[...], 0, n * cap)
    hub_tally = tally[:, :hub_total]
    live_tally = tally[:, hub_total:] * slot_live
    taken = 1.0 + jnp.sum(hub_tally, axis=1, keepdims=True) + jnp.sum(live_tally, axis=1, keepdims=True)
    scale = 1.0 / taken
    hub_tally = hub_tally.astype(jnp.bfloat16)
    for b in range(4):
        slot_tally[b] = live_tally[:, b * quarter * cap : (b + 1) * quarter * cap].astype(jnp.bfloat16)

    take(table, n - 1, local_sem.at[0])
    if reps > 1:
        take(hubs, reps - 1, local_sem.at[2])
        take(hubs, reps - 1, hub_recv_sem.at[0])
    hub_high, hub_low = halves(hubs[...].reshape(hub_total, width))
    total = own[...] + (dot(hub_tally, hub_high) + dot(hub_tally, hub_low))
    weight_high, weight_low = halves(weight[...])

    def add_rows(total, owner_block, count):
        take(fetched, count, row_recv_sem.at[owner_block])
        row_high, row_low = halves(fetched[pl.ds(owner_block * quarter, quarter)].reshape(quarter * cap, width))
        counted = slot_tally[owner_block]
        return total + dot(jnp.concatenate([counted] * 2, axis=1), jnp.concatenate([row_high, row_low], axis=0))

    def project(total):
        mean_high, mean_low = halves(total * scale)
        out_ref[...] = dot(mean_high, weight_high) + (dot(mean_high, weight_low) + dot(mean_low, weight_high))

    total = add_rows(total, block, quarter - 1)
    own[...] = add_rows(total, block + 1 - 2 * lax.rem(block, 2), quarter)

    is_client = ((block == 1) | (block == 2)) & (lax.rem(me, 2) == 0)

    @pl.when(is_client)
    def _():
        take(gathered, n - 2, local_sem.at[1])
        for copy in (*code_copies(), partial_copy):
            copy.wait_send()
        pltpu.make_async_copy(partial_in, partial_in, partial_sem.at[0]).wait()
        project(own[...] + partial_in[...])

    @pl.when(jnp.logical_not(is_client))
    def _():
        take(gathered, n - 1, local_sem.at[1])
        total = own[...]
        for owner_block in (3 - 3 * (block // 2), 2 - block // 2):
            total = add_rows(total, owner_block, quarter)
        project(total)


def local(n, reps, features, seed_self, hub_ids, requests, counts, neighbors, weight, out_bias):
    rows, width = features.shape
    cap = requests.shape[1]
    hub_dev = hub_ids.shape[0]
    seeds, fanout = neighbors.shape
    quarter = n // 4
    hbm = pl.BlockSpec(memory_space=pltpu.HBM)
    dma = pltpu.SemaphoreType.DMA
    product = pl.pallas_call(
        functools.partial(kernel, n, reps),
        out_shape=pltpu.VMEM((seeds, width), jnp.float32),
        in_specs=[hbm] * 7,
        out_specs=pl.BlockSpec(memory_space=pltpu.VMEM),
        scratch_shapes=[
            pltpu.VMEM((rows, width), jnp.float32),
            pltpu.VMEM((seeds, width), jnp.float32),
            pltpu.VMEM(weight.shape, jnp.float32),
            pltpu.VMEM((1, hub_dev), jnp.int32),
            pltpu.VMEM((n, cap), jnp.int32),
            pltpu.VMEM((1, n), jnp.int32),
            pltpu.VMEM((fanout, seeds), jnp.int32),
            pltpu.VMEM((n, 1, LANES), jnp.int32),
            pltpu.VMEM((n, 1, LANES), jnp.int32),
            pltpu.VMEM((rows, width), jnp.bfloat16),
            pltpu.VMEM((rows, width), jnp.bfloat16),
            pltpu.VMEM((n, cap, width), jnp.float32),
            pltpu.VMEM((n, cap, width), jnp.float32),
            pltpu.VMEM((reps, hub_dev, width), jnp.float32),
            pltpu.VMEM((4, seeds, quarter * cap), jnp.bfloat16),
            pltpu.VMEM((2 * quarter, cap, width), jnp.float32),
            pltpu.VMEM((fanout, seeds), jnp.int32),
            pltpu.VMEM((1, n), jnp.int32),
            pltpu.VMEM((seeds, width), jnp.float32),
            pltpu.VMEM((seeds, width), jnp.float32),
            dma((7,)),
            dma((8,)),
            dma((4,)),
            dma((1,)),
            dma((2,)),
            dma((2,)),
            dma((1,)),
        ],
        compiler_params=pltpu.CompilerParams(collective_id=0, has_side_effects=True),
    )(features, seed_self, hub_ids[None], requests, counts[None], neighbors.T, weight)
    return jnp.maximum(product + out_bias, 0.0)


def solution(mesh):
    return jax.shard_map(
        functools.partial(local, mesh.shape["shard"], mesh.shape["rep"]),
        mesh=mesh,
        in_specs=(
            P(("rep", "shard"), None),
            P(("rep", "shard"), None),
            P(("rep", "shard")),
            P(("rep", "shard"), None),
            P(("rep", "shard")),
            P(("rep", "shard"), None),
            P(),
            P(),
        ),
        out_specs=P(("rep", "shard"), None),
        check_vma=False,
    )
```

```python
import functools

import jax
import jax.numpy as jnp
from jax import lax
from jax.experimental import pallas as pl
from jax.experimental.pallas import tpu as pltpu
from jax.sharding import PartitionSpec as P

LANES = 128


def pool_of(peer, quarter):
    block = peer // quarter
    if block in (1, 2) and peer % 2 == 0:
        return peer + (3 - 2 * block) * quarter
    return None


def halves(values):
    high = values.astype(jnp.bfloat16)
    low = (values - high.astype(jnp.float32)).astype(jnp.bfloat16)
    return high, low


def dot(left, right):
    return jnp.dot(left, right, preferred_element_type=jnp.float32)


def columns_of(rows):
    count = rows.shape[0]
    if count % 8:
        rows = jnp.concatenate([rows, jnp.zeros((-count % 8, LANES), rows.dtype)], axis=0)
    return rows.T


def kernel(
    n, reps, feat_hbm, self_hbm, hub_hbm, req_hbm, cnt_hbm, nbr_hbm, weight_hbm, out_ref,
    feat, own, weight, hub_ref, req_ref, cnt_ref, nbr_ref, table, req_recv, high_ref, low_ref, gathered, fetched, hubs, slot_tally,
    pool, pool_codes, pool_counts, partial, partial_in,
    local_sem, ask_recv_sem, row_recv_sem, hub_recv_sem, pool_sem, code_recv_sem, partial_sem,
):
    me = lax.axis_index("shard")
    rep = lax.axis_index("rep")
    rows, width = feat.shape
    cap = req_ref.shape[1]
    hub_dev = hub_ref.shape[1]
    fanout, seeds = nbr_ref.shape
    hub_total = hub_dev * reps
    quarter = n // 4
    block, place = me // quarter, lax.rem(me, quarter)

    barrier = pltpu.get_barrier_semaphore()
    for off in range(1, n):
        pl.semaphore_signal(barrier, inc=1, device_id={"shard": lax.rem(me + off, n)})
    for off in range(1, reps):
        pl.semaphore_signal(barrier, inc=1, device_id={"rep": lax.rem(rep + off, reps)})

    loads = [
        pltpu.make_async_copy(src, dst, local_sem.at[i])
        for i, (src, dst) in enumerate(
            (
                (req_hbm, req_ref),
                (feat_hbm, feat),
                (hub_hbm, hub_ref),
                (nbr_hbm, nbr_ref),
                (cnt_hbm, cnt_ref),
                (self_hbm, own),
                (weight_hbm, weight),
            )
        )
    ]
    for load in loads:
        load.start()

    loads[0].wait()
    lists = jnp.concatenate([req_ref[...], jnp.zeros((n, LANES - cap), jnp.int32)], axis=1)
    table[...] = lists.reshape(n, 1, LANES)
    req_recv[me] = table[me]

    row_iota = lax.broadcasted_iota(jnp.int32, (LANES, rows), 1)

    def split():
        for load in (loads[1], loads[5], loads[6]):
            load.wait()
        high_ref[...], low_ref[...] = halves(feat[...])

    def gather(pick):
        pick = pick.astype(jnp.float32).astype(jnp.bfloat16)
        return dot(pick, high_ref[...]) + dot(pick, low_ref[...])

    def gather_hubs():
        loads[2].wait()
        hub_columns = columns_of(jnp.broadcast_to(hub_ref[...], (8, hub_dev)))
        hubs[rep] = gather(hub_columns[:, 0:1] == row_iota)

    def enter():
        pl.semaphore_wait(barrier, n - 1 + reps - 1)

    loads[3].wait()
    loads[4].wait()

    def ask_copy(peer):
        return pltpu.make_async_remote_copy(
            src_ref=table.at[peer],
            dst_ref=req_recv.at[me],
            send_sem=local_sem.at[0],
            recv_sem=ask_recv_sem.at[2 * block + lax.rem(me, 2)],
            device_id={"shard": peer},
        )

    def ask(own_block, to_block):
        for spot in (*range(1, quarter, 2), *range(0, quarter, 2)):
            peer = to_block * quarter + spot
            if to_block != own_block:
                ask_copy(peer).start()
                continue

            @pl.when(spot != place)
            def _():
                ask_copy(peer).start()

    def code_copies():
        peer = (3 - block) * quarter + place
        return [
            pltpu.make_async_remote_copy(
                src_ref=src,
                dst_ref=dst,
                send_sem=local_sem.at[3 + i],
                recv_sem=code_recv_sem.at[i],
                device_id={"shard": peer},
            )
            for i, (src, dst) in enumerate(((nbr_ref, pool_codes), (cnt_ref, pool_counts)))
        ]

    def send_codes():
        for copy in code_copies():
            copy.start()

    def share_copy(other):
        return pltpu.make_async_remote_copy(
            src_ref=hubs.at[rep],
            dst_ref=hubs.at[rep],
            send_sem=local_sem.at[2],
            recv_sem=hub_recv_sem.at[0],
            device_id={"rep": other},
        )

    def share():
        for other in range(reps):

            @pl.when(other != rep)
            def _():
                share_copy(other).start()

    def take(buffer, count, sem):
        part = buffer.at[pl.ds(0, count)]
        pltpu.make_async_copy(part, part, sem).wait()

    batch = min(LANES // cap, quarter)

    def reply_copy(peer):
        return pltpu.make_async_remote_copy(
            src_ref=gathered.at[peer],
            dst_ref=fetched.at[me],
            send_sem=local_sem.at[1],
            recv_sem=row_recv_sem.at[block],
            device_id={"shard": peer},
        )

    def answer(own_block, peer_block, places):
        peers = [peer_block * quarter + spot for spot in places]

        def unless_me(peer, action):
            if peer_block == own_block:
                pl.when(peer != me)(action)
            else:
                action()

        for parity in sorted({spot % 2 for spot in places}):
            sem = ask_recv_sem.at[2 * peer_block + parity]
            count = quarter // 2
            if peer_block != own_block:
                take(req_recv, count, sem)
                continue

            @pl.when(lax.rem(me, 2) == parity)
            def _():
                take(req_recv, count - 1, sem)

            @pl.when(lax.rem(me, 2) != parity)
            def _():
                take(req_recv, count, sem)

        request_columns = columns_of(jnp.concatenate([req_recv[peer] for peer in peers], axis=0))
        for first in range(0, len(peers), batch):
            group = peers[first : first + batch]
            picked = gather(
                jnp.concatenate(
                    [
                        request_columns[:cap, i : i + 1] == row_iota[:cap]
                        for i in range(first, first + len(group))
                    ],
                    axis=0,
                )
            )
            for i, peer in enumerate(group):
                gathered[peer] = picked[i * cap : (i + 1) * cap]
            for peer in group:
                pool_peer = pool_of(peer, quarter)
                if pool_peer is not None and own_block // 2 != peer_block // 2:
                    row = lax.rem(me, 2 * quarter)
                    forward = pltpu.make_async_remote_copy(
                        src_ref=gathered.at[peer],
                        dst_ref=pool.at[row],
                        send_sem=local_sem.at[1],
                        recv_sem=pool_sem.at[lax.rem(block, 2)],
                        device_id={"shard": pool_peer},
                    )
                    if own_block == 3 - peer_block:
                        pl.when(pool_peer != me)(forward.start)
                    else:
                        forward.start()
                else:
                    unless_me(peer, reply_copy(peer).start)

    def tally_of(codes, low, count):
        code_iota = low + lax.broadcasted_iota(jnp.int32, (seeds, count), 1)
        tally = jnp.zeros((seeds, count), jnp.float32)
        for k in range(fanout):
            tally = tally + (codes[:, k : k + 1] == code_iota).astype(jnp.float32)
        return tally

    def live_of(counts, low, count):
        spread = (
            low // cap + lax.broadcasted_iota(jnp.int32, (n, count), 1) // cap
            == lax.broadcasted_iota(jnp.int32, (n, count), 0)
        ).astype(jnp.float32).astype(jnp.bfloat16)
        fill = jnp.broadcast_to(counts.astype(jnp.float32), (8, n)).astype(jnp.bfloat16)
        slot_iota = (lax.broadcasted_iota(jnp.int32, (1, count), 1) % cap).astype(jnp.float32)
        return (slot_iota < dot(fill, spread)[0:1]).astype(jnp.float32)

    partial_copy = pltpu.make_async_remote_copy(
        src_ref=partial,
        dst_ref=partial_in,
        send_sem=local_sem.at[5],
        recv_sem=partial_sem.at[0],
        device_id={"shard": (3 - block) * quarter + place},
    )

    def pool_rows(own_block):
        for i, ref in enumerate((pool_codes, pool_counts)):
            pltpu.make_async_copy(ref, ref, code_recv_sem.at[i]).wait()
        low = own_block // 2 * 2 * quarter * cap
        part = quarter * cap
        counted = tally_of(columns_of(pool_codes[...]), hub_total + low, 2 * part)
        counted = (counted * live_of(pool_counts[...], low, 2 * part)).astype(jnp.bfloat16)
        pool[lax.rem(me, 2 * quarter)] = gathered[(3 - own_block) * quarter + place]
        total = None
        own_part = own_block % 2
        for i in (own_part, 1 - own_part):
            take(pool, quarter - 1 if i == own_part else quarter, pool_sem.at[i])
            row_high, row_low = halves(pool[i * quarter : (i + 1) * quarter].reshape(part, width))
            chosen = counted[:, i * part : (i + 1) * part]
            term = dot(chosen, row_high) + dot(chosen, row_low)
            total = term if total is None else total + term
        partial[...] = total
        partial_copy.start()

    every, odd, even = range(quarter), range(1, quarter, 2), range(0, quarter, 2)
    front, back = range(quarter // 2), range(quarter // 2, quarter)
    @pl.when(block == 0)
    def _():
        split()
        gather_hubs()
        enter()
        ask(0, 3)
        ask(0, 2)
        ask(0, 1)
        ask(0, 0)
        share()
        answer(0, 2, even)
        answer(0, 0, every)
        answer(0, 3, every)
        answer(0, 1, every)
        answer(0, 2, odd)

    @pl.when(block == 1)
    def _():
        split()
        gather_hubs()
        enter()
        ask(1, 3)
        ask(1, 0)
        ask(1, 2)
        pl.when(lax.rem(me, 2) == 0)(send_codes)
        ask(1, 1)
        answer(1, 2, odd)
        answer(1, 0, every)
        answer(1, 2, even)
        share()
        answer(1, 3, every)
        answer(1, 1, every)
        pl.when(lax.rem(me, 2) == 0)(functools.partial(pool_rows, 1))

    @pl.when(block == 2)
    def _():
        split()
        enter()
        ask(2, 0)
        ask(2, 1)
        pl.when(lax.rem(me, 2) == 0)(send_codes)
        ask(2, 2)
        ask(2, 3)
        gather_hubs()
        share()
        answer(2, 1, odd)
        answer(2, 1, even)
        answer(2, 0, every)
        answer(2, 2, every)
        answer(2, 3, every)
        pl.when(lax.rem(me, 2) == 0)(functools.partial(pool_rows, 2))

    @pl.when(block == 3)
    def _():
        enter()
        ask(3, 0)
        ask(3, 1)
        ask(3, 2)
        ask(3, 3)
        split()
        gather_hubs()
        answer(3, 3, every)
        answer(3, 1, even)
        answer(3, 1, odd)
        share()
        answer(3, 0, every)
        answer(3, 2, every)

    fetched[me] = gathered[me]

    tally = tally_of(columns_of(nbr_ref[...]), 0, hub_total + n * cap)
    slot_live = live_of(cnt_ref[...], 0, n * cap)
    hub_tally = tally[:, :hub_total]
    live_tally = tally[:, hub_total:] * slot_live
    taken = 1.0 + jnp.sum(hub_tally, axis=1, keepdims=True) + jnp.sum(live_tally, axis=1, keepdims=True)
    scale = 1.0 / taken
    hub_tally = hub_tally.astype(jnp.bfloat16)
    for b in range(4):
        slot_tally[b] = live_tally[:, b * quarter * cap : (b + 1) * quarter * cap].astype(jnp.bfloat16)

    take(table, n - 1, local_sem.at[0])
    if reps > 1:
        take(hubs, reps - 1, local_sem.at[2])
        take(hubs, reps - 1, hub_recv_sem.at[0])
    hub_high, hub_low = halves(hubs[...].reshape(hub_total, width))
    total = own[...] + (dot(hub_tally, hub_high) + dot(hub_tally, hub_low))
    weight_high, weight_low = halves(weight[...])

    def add_rows(total, owner_block, count):
        take(fetched, count, row_recv_sem.at[owner_block])
        row_high, row_low = halves(fetched[pl.ds(owner_block * quarter, quarter)].reshape(quarter * cap, width))
        counted = slot_tally[owner_block]
        return total + dot(jnp.concatenate([counted] * 2, axis=1), jnp.concatenate([row_high, row_low], axis=0))

    def project(total):
        mean_high, mean_low = halves(total * scale)
        out_ref[...] = dot(mean_high, weight_high) + (dot(mean_high, weight_low) + dot(mean_low, weight_high))

    total = add_rows(total, block, quarter - 1)
    own[...] = add_rows(total, block + 1 - 2 * lax.rem(block, 2), quarter)

    is_client = ((block == 1) | (block == 2)) & (lax.rem(me, 2) == 0)

    @pl.when(is_client)
    def _():
        take(gathered, n - 2, local_sem.at[1])
        for copy in (*code_copies(), partial_copy):
            copy.wait_send()
        pltpu.make_async_copy(partial_in, partial_in, partial_sem.at[0]).wait()
        project(own[...] + partial_in[...])

    @pl.when(jnp.logical_not(is_client))
    def _():
        take(gathered, n - 1, local_sem.at[1])
        total = own[...]
        for owner_block in (3 - 3 * (block // 2), 2 - block // 2):
            total = add_rows(total, owner_block, quarter)
        project(total)


def local(n, reps, features, seed_self, hub_ids, requests, counts, neighbors, weight, out_bias):
    rows, width = features.shape
    cap = requests.shape[1]
    hub_dev = hub_ids.shape[0]
    seeds, fanout = neighbors.shape
    quarter = n // 4
    hbm = pl.BlockSpec(memory_space=pltpu.HBM)
    dma = pltpu.SemaphoreType.DMA
    product = pl.pallas_call(
        functools.partial(kernel, n, reps),
        out_shape=pltpu.VMEM((seeds, width), jnp.float32),
        in_specs=[hbm] * 7,
        out_specs=pl.BlockSpec(memory_space=pltpu.VMEM),
        scratch_shapes=[
            pltpu.VMEM((rows, width), jnp.float32),
            pltpu.VMEM((seeds, width), jnp.float32),
            pltpu.VMEM(weight.shape, jnp.float32),
            pltpu.VMEM((1, hub_dev), jnp.int32),
            pltpu.VMEM((n, cap), jnp.int32),
            pltpu.VMEM((1, n), jnp.int32),
            pltpu.VMEM((fanout, seeds), jnp.int32),
            pltpu.VMEM((n, 1, LANES), jnp.int32),
            pltpu.VMEM((n, 1, LANES), jnp.int32),
            pltpu.VMEM((rows, width), jnp.bfloat16),
            pltpu.VMEM((rows, width), jnp.bfloat16),
            pltpu.VMEM((n, cap, width), jnp.float32),
            pltpu.VMEM((n, cap, width), jnp.float32),
            pltpu.VMEM((reps, hub_dev, width), jnp.float32),
            pltpu.VMEM((4, seeds, quarter * cap), jnp.bfloat16),
            pltpu.VMEM((2 * quarter, cap, width), jnp.float32),
            pltpu.VMEM((fanout, seeds), jnp.int32),
            pltpu.VMEM((1, n), jnp.int32),
            pltpu.VMEM((seeds, width), jnp.float32),
            pltpu.VMEM((seeds, width), jnp.float32),
            dma((7,)),
            dma((8,)),
            dma((4,)),
            dma((1,)),
            dma((2,)),
            dma((2,)),
            dma((1,)),
        ],
        compiler_params=pltpu.CompilerParams(
            collective_id=0, has_side_effects=True
        ),
    )(features, seed_self, hub_ids[None], requests, counts[None], neighbors.T, weight)
    return jnp.maximum(product + out_bias, 0.0)


def solution(mesh):
    return jax.shard_map(
        functools.partial(local, mesh.shape["shard"], mesh.shape["rep"]),
        mesh=mesh,
        in_specs=(
            P(("rep", "shard"), None),
            P(("rep", "shard"), None),
            P(("rep", "shard")),
            P(("rep", "shard"), None),
            P(("rep", "shard")),
            P(("rep", "shard"), None),
            P(),
            P(),
        ),
        out_specs=P(("rep", "shard"), None),
        check_vma=False,
    )
```
